32 devices in a mesh: seq: 4 (over y, core), head: 8 (over z, x).
Axes of the slice: x: 2, y: 2, z: 4, core: 2. Of those that a mesh axis runs over, the one named last changes fastest.
Arguments:
- query: bfloat16 [4096, 4096], P(('seq', 'head')), may hold values from -6 to 6
- key_matrix: bfloat16 [4096, 2048], P(('seq', 'head')), may hold values from -6 to 6
- value_matrix: bfloat16 [4096, 2048], P(('seq', 'head')), may hold values from -6 to 6
- output_gradient: bfloat16 [4096, 4096], P(('seq', 'head')), may hold values from -6 to 6
- attn_out: bfloat16 [4096, 4096], P(('seq', 'head')), may hold values from -3 to 3
- doc_offsets: int32 [9], replicated, may hold values from 0 to 4096, as said below
- stats: float32 [4096, 32], P(('seq', 'head')), may hold values from -1 to 9
Outputs:
- grad_query: bfloat16 [4096, 4096], P(('seq', 'head'))
- key_gradient: bfloat16 [4096, 2048], P(('seq', 'head'))
- value_gradient: bfloat16 [4096, 2048], P(('seq', 'head'))
The draws below stay inside these ranges and needn't reach their ends.
Inputs may be any that keep to these rules, and one draw needn't show every extreme that they name: doc_offsets[0] is 0, doc_offsets[8] is 4096, the entries rise strictly; no document has more than 1023 tokens and one has exactly that many.
All inputs are finite; a program needn't handle non-finite values.
Results may differ from the reference program's by a relative error of at most 0.0063.
Values may be sent and summed in bfloat16 or wider, within the bound.
A program may use at most 64 MiB of HBM per device.

```python
import jax
import jax.numpy as jnp
from jax import lax

HQ = 32
KEY_VALUE_HEADS = 16
HEAD_SIZE = 128
DOCHALF = 512
QBLK = 512
PACKED_TOKENS = 4096


def doc_bounds(key):
    frames = PACKED_TOKENS // DOCHALF
    base = jax.random.fold_in(key, 101)
    cut_key, pick_key = jax.random.split(base)
    index = jnp.arange(1, frames, dtype=jnp.int32)
    cuts = jax.random.randint(cut_key, (frames - 1,), 0, DOCHALF, dtype=jnp.int32)
    chosen = jax.random.randint(pick_key, (), 1, frames - 1, dtype=jnp.int32)
    cuts = jnp.where(index == chosen, 0, cuts)
    cuts = jnp.where(index == chosen + 1, DOCHALF - 1, cuts)
    inner = index * DOCHALF + cuts
    return jnp.concatenate([jnp.zeros((1,), jnp.int32), inner, jnp.full((1,), PACKED_TOKENS, jnp.int32)])


def draw_doc_offsets(key, part):
    return doc_bounds(key)


def draw_stats(key, part):
    bounds = doc_bounds(key)
    positions = jnp.arange(PACKED_TOKENS, dtype=jnp.int32)
    number = jnp.sum((bounds[1:-1][None, :] <= positions[:, None]).astype(jnp.int32), axis=1)
    starts = bounds[number]
    visible = (positions - starts + 1).astype(jnp.float32)
    noise_key = jax.random.fold_in(key, 202)
    spread = jax.random.uniform(noise_key, (PACKED_TOKENS, HQ), jnp.float32, -0.3, 0.3)
    return jnp.log(visible)[:, None] + 0.44 + spread


def level_of(own_key, shape, shards, least, largest):
    gain = 1.0
    for position, blocks in shards:
        draws = jax.random.uniform(jax.random.fold_in(jax.random.fold_in(own_key, 6), position), (blocks,), jnp.float32, least / len(shards), largest / len(shards))
        gain = gain * jnp.repeat(jnp.exp(draws), shape[position] // blocks).reshape((-1,) + (1,) * (len(shape) - 1 - position))
    return gain


def noise(key, extent, scale, most, cuts=(), kind=jnp.bfloat16):
    entries = scale * jax.random.normal(key, extent, jnp.float32)
    if cuts:
        entries = entries * level_of(key, extent, cuts, -0.22, 0.18)
    return jnp.clip(entries, -most, most).astype(kind)


def setup_inputs(seed: int = 0) -> dict:
    keys = jax.random.split(jax.random.key(seed), 8)
    return {
        "query": noise(keys[0], (PACKED_TOKENS, HQ * HEAD_SIZE), 1.0, 6.0, ((0, 32),)),
        "key_matrix": noise(keys[1], (PACKED_TOKENS, KEY_VALUE_HEADS * HEAD_SIZE), 1.0, 6.0, ((0, 32),)),
        "value_matrix": noise(keys[2], (PACKED_TOKENS, KEY_VALUE_HEADS * HEAD_SIZE), 1.0, 6.0, ((0, 32),)),
        "output_gradient": noise(keys[3], (PACKED_TOKENS, HQ * HEAD_SIZE), 1.0, 6.0, ((0, 32),)),
        "attn_out": noise(keys[4], (PACKED_TOKENS, HQ * HEAD_SIZE), 0.5, 3.0, ((0, 32),)),
        "doc_offsets": draw_doc_offsets(jax.random.fold_in(keys[7], 71), 0),
        "stats": draw_stats(jax.random.fold_in(keys[7], 71), 0),
    }


attn_scale = 144.0 ** -0.5


def tile_grads(query_rows, grad_rows, lse_rows, delta_rows, key_window, value_window, allowed):
    query_wide = query_rows.astype(jnp.float32)
    grad_wide = grad_rows.astype(jnp.float32)
    key_wide = key_window.astype(jnp.float32)
    value_wide = value_window.astype(jnp.float32)
    score = jnp.einsum("qgrd,kgd->grqk", query_wide, key_wide) * attn_scale
    norm_stat = jnp.transpose(lse_rows, (1, 2, 0))[..., None]
    prob = jnp.where(allowed[None, None], jnp.exp(score - norm_stat), 0.0)
    dprob = jnp.einsum("qgrd,kgd->grqk", grad_wide, value_wide)
    dscore = prob * (dprob - jnp.transpose(delta_rows, (1, 2, 0))[..., None])
    prob_low = prob.astype(jnp.bfloat16).astype(jnp.float32)
    dscore_low = dscore.astype(jnp.bfloat16).astype(jnp.float32)
    value_gradient = jnp.einsum("grqk,qgrd->kgd", prob_low, grad_wide)
    key_gradient = jnp.einsum("grqk,qgrd->kgd", dscore_low, query_wide) * attn_scale
    grad_query = jnp.einsum("grqk,kgd->qgrd", dscore_low, key_wide) * attn_scale
    return grad_query, key_gradient, value_gradient


def doc_numbers(positions, inner):
    return jnp.sum((inner[None, :] <= positions[:, None]).astype(jnp.int32), axis=1)


def reference(query, key_matrix, value_matrix, output_gradient, attn_out, doc_offsets, stats):
    lookback = 2 * DOCHALF
    width = lookback + QBLK
    inner = doc_offsets[1:-1]
    query_pos = jnp.arange(PACKED_TOKENS, dtype=jnp.int32)
    key_pos = jnp.arange(PACKED_TOKENS + lookback, dtype=jnp.int32) - lookback
    query_doc = doc_numbers(query_pos, inner)
    key_doc = doc_numbers(key_pos, inner)
    delta_correction = jnp.sum((output_gradient.astype(jnp.float32) * attn_out.astype(jnp.float32)).reshape(PACKED_TOKENS, HQ, HEAD_SIZE), axis=2)
    query_grouped = query.reshape(PACKED_TOKENS, KEY_VALUE_HEADS, 2, HEAD_SIZE)
    output_gradient_grouped = output_gradient.reshape(PACKED_TOKENS, KEY_VALUE_HEADS, 2, HEAD_SIZE)
    key_cube = key_matrix.reshape(PACKED_TOKENS, KEY_VALUE_HEADS, HEAD_SIZE)
    value_cube = value_matrix.reshape(PACKED_TOKENS, KEY_VALUE_HEADS, HEAD_SIZE)
    logsumexp_cube = stats.reshape(PACKED_TOKENS, KEY_VALUE_HEADS, 2)
    delta_correction_cube = delta_correction.reshape(PACKED_TOKENS, KEY_VALUE_HEADS, 2)
    padding = jnp.zeros((lookback, 1, HEAD_SIZE), jnp.bfloat16)

    def single_head_slice(head):
        query_head = query_grouped[:, head][:, None]
        grad_head = output_gradient_grouped[:, head][:, None]
        lse_head = logsumexp_cube[:, head][:, None]
        delta_head = delta_correction_cube[:, head][:, None]
        key_ext = jnp.concatenate([padding, key_cube[:, head][:, None]], 0)
        value_ext = jnp.concatenate([padding, value_cube[:, head][:, None]], 0)

        def block_step(block, carry):
            grad_q, grad_k, grad_v = carry
            start = (block * QBLK).astype(jnp.int32)
            query_rows = lax.dynamic_slice_in_dim(query_head, start, QBLK, 0)
            grad_rows = lax.dynamic_slice_in_dim(grad_head, start, QBLK, 0)
            lse_rows = lax.dynamic_slice_in_dim(lse_head, start, QBLK, 0)
            delta_rows = lax.dynamic_slice_in_dim(delta_head, start, QBLK, 0)
            key_window = lax.dynamic_slice_in_dim(key_ext, start, width, 0)
            value_window = lax.dynamic_slice_in_dim(value_ext, start, width, 0)
            rows_pos = lax.dynamic_slice_in_dim(query_pos, start, QBLK, 0)
            rows_doc = lax.dynamic_slice_in_dim(query_doc, start, QBLK, 0)
            cols_pos = lax.dynamic_slice_in_dim(key_pos, start, width, 0)
            cols_doc = lax.dynamic_slice_in_dim(key_doc, start, width, 0)
            allowed = (cols_doc[None, :] == rows_doc[:, None]) & (cols_pos[None, :] <= rows_pos[:, None]) & (cols_pos[None, :] >= 0)
            block_q, block_k, block_v = tile_grads(query_rows, grad_rows, lse_rows, delta_rows, key_window, value_window, allowed)
            grad_q = lax.dynamic_update_slice_in_dim(grad_q, block_q, start, 0)
            grad_k = lax.dynamic_update_slice_in_dim(grad_k, lax.dynamic_slice_in_dim(grad_k, start, width, 0) + block_k, start, 0)
            grad_v = lax.dynamic_update_slice_in_dim(grad_v, lax.dynamic_slice_in_dim(grad_v, start, width, 0) + block_v, start, 0)
            return grad_q, grad_k, grad_v

        init = (jnp.zeros((PACKED_TOKENS, 1, 2, HEAD_SIZE), jnp.float32), jnp.zeros((PACKED_TOKENS + lookback, 1, HEAD_SIZE), jnp.float32), jnp.zeros((PACKED_TOKENS + lookback, 1, HEAD_SIZE), jnp.float32))
        grad_q, grad_k, grad_v = lax.fori_loop(0, PACKED_TOKENS // QBLK, block_step, init)
        return grad_q[:, 0], grad_k[lookback:, 0], grad_v[lookback:, 0]

    every_query_row, every_key_row, every_value_row = lax.map(single_head_slice, jnp.arange(KEY_VALUE_HEADS, dtype=jnp.int32))
    grad_query = jnp.transpose(every_query_row, (1, 0, 2, 3)).reshape(PACKED_TOKENS, HQ * HEAD_SIZE).astype(jnp.bfloat16)
    key_gradient = jnp.transpose(every_key_row, (1, 0, 2)).reshape(PACKED_TOKENS, KEY_VALUE_HEADS * HEAD_SIZE).astype(jnp.bfloat16)
    value_gradient = jnp.transpose(every_value_row, (1, 0, 2)).reshape(PACKED_TOKENS, KEY_VALUE_HEADS * HEAD_SIZE).astype(jnp.bfloat16)
    return (grad_query, key_gradient, value_gradient)
```

```python
import functools
import math

import jax
import jax.numpy as jnp
from jax import lax
from jax.experimental import pallas as pl
from jax.experimental.pallas import tpu as pltpu
from jax.sharding import PartitionSpec as P

HQ = 32
HEAD_SIZE = 128
DOCHALF = 512
QBLK = 512


attn_scale = 144.0 ** (-0.5)


def partner(value, axis, apart):
    mask = 2**apart
    pairs = [(source, source ^ mask) for source in range(lax.axis_size(axis))]
    return lax.ppermute(value, axis, pairs)


def from_behind(value, axis, steps):
    count = lax.axis_size(axis)
    leading, last = (max(0, -steps), min(count, count - steps))
    return lax.ppermute(value, axis, [(source, source + steps) for source in range(leading, last)])


def tile_grads(query_rows, grad_rows, lse_rows, delta_rows, key_window, value_window, allowed):
    score = (
        jnp.einsum("qgrd,kgd->grqk", query_rows, key_window, preferred_element_type=jnp.float32)
        * attn_scale
    )
    norm_stat = jnp.transpose(lse_rows, (1, 2, 0))[..., None]
    prob = jnp.where(allowed[None, None], jnp.exp(score - norm_stat), 0.0)
    dprob = jnp.einsum(
        "qgrd,kgd->grqk", grad_rows, value_window, preferred_element_type=jnp.float32
    )
    dscore = prob * (dprob - jnp.transpose(delta_rows, (1, 2, 0))[..., None])
    prob_low = prob.astype(jnp.bfloat16)
    dscore_low = dscore.astype(jnp.bfloat16)
    value_gradient = jnp.einsum(
        "grqk,qgrd->kgd", prob_low, grad_rows, preferred_element_type=jnp.float32
    )
    key_gradient = (
        jnp.einsum("grqk,qgrd->kgd", dscore_low, query_rows, preferred_element_type=jnp.float32)
        * attn_scale
    )
    grad_query = (
        jnp.einsum("grqk,kgd->qgrd", dscore_low, key_window, preferred_element_type=jnp.float32)
        * attn_scale
    )
    return (grad_query, key_gradient, value_gradient)


def doc_numbers(positions, inner):
    return jnp.sum((inner[None, :] <= positions[:, None]).astype(jnp.int32), axis=1)


def shards(query, key_matrix, value_matrix, output_gradient, attn_out, doc_offsets, stats):
    token_count_local = query.shape[0]
    members = lax.axis_size("head")
    group_span = token_count_local * members
    per_device = HQ // members
    lookback = 2 * DOCHALF
    width = lookback + QBLK
    group = lax.axis_index("seq")
    member = lax.axis_index("head")
    parity = member % 2
    half_width = HEAD_SIZE // 2
    delta_correction = jnp.sum(
        (output_gradient.astype(jnp.float32) * attn_out.astype(jnp.float32)).reshape(
            token_count_local, HQ, HEAD_SIZE
        ),
        axis=2,
    )
    query_heads, grad_heads = (
        lax.all_to_all(query, "head", split_axis=1, concat_axis=0, tiled=True),
        lax.all_to_all(output_gradient, "head", split_axis=1, concat_axis=0, tiled=True),
    )
    lse_heads, delta_heads = (
        lax.all_to_all(stats, "head", split_axis=1, concat_axis=0, tiled=True),
        lax.all_to_all(delta_correction, "head", split_axis=1, concat_axis=0, tiled=True),
    )
    key_cols, value_cols = (
        lax.all_to_all(key_matrix, "head", split_axis=1, concat_axis=0, tiled=True),
        lax.all_to_all(value_matrix, "head", split_axis=1, concat_axis=0, tiled=True),
    )
    if per_device >= 2:
        groups = per_device // 2
        key_heads = key_cols.reshape(group_span, groups, HEAD_SIZE)
        value_heads = value_cols.reshape(group_span, groups, HEAD_SIZE)
    else:
        groups = 1
        other_key, other_value = partner((key_cols, value_cols), "head", 0)
        key_heads = jnp.where(
            parity == 0,
            jnp.concatenate([key_cols, other_key], 1),
            jnp.concatenate([other_key, key_cols], 1),
        ).reshape(group_span, 1, HEAD_SIZE)
        value_heads = jnp.where(
            parity == 0,
            jnp.concatenate([value_cols, other_value], 1),
            jnp.concatenate([other_value, value_cols], 1),
        ).reshape(group_span, 1, HEAD_SIZE)
    repeats = per_device // groups
    query_heads = query_heads.reshape(group_span, groups, repeats, HEAD_SIZE)
    grad_heads = grad_heads.reshape(group_span, groups, repeats, HEAD_SIZE)
    lse_heads = lse_heads.reshape(group_span, groups, repeats)
    delta_heads = delta_heads.reshape(group_span, groups, repeats)
    prior_key, prior_value = from_behind(
        (key_heads[group_span - lookback :], value_heads[group_span - lookback :]), "seq", 1
    )
    key_ext = jnp.concatenate([prior_key, key_heads], 0)
    value_ext = jnp.concatenate([prior_value, value_heads], 0)
    inner = doc_offsets[1:-1]
    query_pos = group * group_span + jnp.arange(group_span, dtype=jnp.int32)
    key_pos = group * group_span - lookback + jnp.arange(lookback + group_span, dtype=jnp.int32)
    query_doc = doc_numbers(query_pos, inner)
    key_doc = doc_numbers(key_pos, inner)

    def block_step(block, carry):
        grad_q, grad_k, grad_v = carry
        start = (block * QBLK).astype(jnp.int32)
        query_rows = lax.dynamic_slice_in_dim(query_heads, start, QBLK, 0)
        grad_rows = lax.dynamic_slice_in_dim(grad_heads, start, QBLK, 0)
        lse_rows = lax.dynamic_slice_in_dim(lse_heads, start, QBLK, 0)
        delta_rows = lax.dynamic_slice_in_dim(delta_heads, start, QBLK, 0)
        key_window = lax.dynamic_slice_in_dim(key_ext, start, width, 0)
        value_window = lax.dynamic_slice_in_dim(value_ext, start, width, 0)
        rows_pos = lax.dynamic_slice_in_dim(query_pos, start, QBLK, 0)
        rows_doc = lax.dynamic_slice_in_dim(query_doc, start, QBLK, 0)
        cols_pos = lax.dynamic_slice_in_dim(key_pos, start, width, 0)
        cols_doc = lax.dynamic_slice_in_dim(key_doc, start, width, 0)
        allowed = (
            (cols_doc[None, :] == rows_doc[:, None])
            & (cols_pos[None, :] <= rows_pos[:, None])
            & (cols_pos[None, :] >= 0)
        )
        block_q, block_k, block_v = tile_grads(
            query_rows, grad_rows, lse_rows, delta_rows, key_window, value_window, allowed
        )
        grad_q = lax.dynamic_update_slice_in_dim(grad_q, block_q, start, 0)
        grad_k = lax.dynamic_update_slice_in_dim(
            grad_k, lax.dynamic_slice_in_dim(grad_k, start, width, 0) + block_k, start, 0
        )
        grad_v = lax.dynamic_update_slice_in_dim(
            grad_v, lax.dynamic_slice_in_dim(grad_v, start, width, 0) + block_v, start, 0
        )
        return (grad_q, grad_k, grad_v)

    init = (
        jnp.zeros((group_span, groups, repeats, HEAD_SIZE), jnp.float32),
        jnp.zeros((lookback + group_span, groups, HEAD_SIZE), jnp.float32),
        jnp.zeros((lookback + group_span, groups, HEAD_SIZE), jnp.float32),
    )
    grad_q, grad_k, grad_v = lax.fori_loop(0, group_span // QBLK, block_step, init)
    back_key, back_value = (
        from_behind(grad_k[:lookback].astype(jnp.bfloat16), "seq", -1).astype(jnp.float32),
        from_behind(grad_v[:lookback].astype(jnp.bfloat16), "seq", -1).astype(jnp.float32),
    )
    own_key = grad_k[lookback:].at[group_span - lookback :].add(back_key)
    own_value = grad_v[lookback:].at[group_span - lookback :].add(back_value)
    query_low = grad_q.astype(jnp.bfloat16).reshape(group_span, per_device * HEAD_SIZE)
    grad_query = lax.all_to_all(query_low, "head", split_axis=0, concat_axis=1, tiled=True)
    if per_device >= 2:
        send_key = own_key.reshape(group_span, groups * HEAD_SIZE)
        send_value = own_value.reshape(group_span, groups * HEAD_SIZE)
    else:
        flat_key = own_key.reshape(group_span, HEAD_SIZE)
        flat_value = own_value.reshape(group_span, HEAD_SIZE)
        keep_key = lax.dynamic_slice_in_dim(flat_key, parity * half_width, half_width, 1)
        keep_value = lax.dynamic_slice_in_dim(flat_value, parity * half_width, half_width, 1)
        give_key = lax.dynamic_slice_in_dim(flat_key, (1 - parity) * half_width, half_width, 1)
        give_value = lax.dynamic_slice_in_dim(flat_value, (1 - parity) * half_width, half_width, 1)
        from_key, from_value = partner((give_key, give_value), "head", 0)
        send_key = keep_key + from_key
        send_value = keep_value + from_value
    key_gradient_summed, value_gradient_summed = (
        lax.all_to_all(
            send_key.astype(jnp.bfloat16), "head", split_axis=0, concat_axis=1, tiled=True
        ).astype(send_key.dtype),
        lax.all_to_all(
            send_value.astype(jnp.bfloat16), "head", split_axis=0, concat_axis=1, tiled=True
        ).astype(send_value.dtype),
    )
    key_gradient = key_gradient_summed.astype(jnp.bfloat16)
    value_gradient = value_gradient_summed.astype(jnp.bfloat16)
    return (grad_query, key_gradient, value_gradient)


TOKENS = 128
TILE = 256
MESH = pl.DeviceIdType.MESH


def wait_bytes(ref, sem):
    pltpu.make_async_copy(ref, ref, sem).wait()


def greet_all(groups, members, group, member):
    barrier = pltpu.get_barrier_semaphore()
    everyone = groups * members

    @pl.loop(1, everyone)
    def _(apart):
        to_group = lax.rem(group + apart // members, groups)
        to_member = lax.rem(member + lax.rem(apart, members), members)
        pl.semaphore_signal(barrier, inc=1, device_id=(to_group, to_member), device_id_type=MESH)

    pl.semaphore_wait(barrier, everyone - 1)


def spread_kernel(
    groups,
    members,
    query,
    grad,
    key,
    value,
    stat,
    query_all,
    grad_all,
    key_all,
    value_all,
    stat_all,
    send_sem,
    recv_sem,
):
    half = members // 2
    everyone = groups * members
    group = lax.axis_index("seq")
    member = lax.axis_index("head")
    side = member // half
    greet_all(groups, members, group, member)
    token_row = pl.multiple_of((group * members + member) * TOKENS, TOKENS)
    side_slot = group * half + lax.rem(member, half)
    side_row = pl.multiple_of(side_slot * TOKENS, TOKENS)

    def pieces(slot):
        narrow = pl.ds(pl.multiple_of(slot * HEAD_SIZE, HEAD_SIZE), HEAD_SIZE)
        wide = pl.ds(pl.multiple_of(slot * 2 * HEAD_SIZE, 2 * HEAD_SIZE), 2 * HEAD_SIZE)
        far = (
            (key.at[:, narrow], key_all.at[pl.ds(token_row, TOKENS)], 0),
            (value.at[:, narrow], value_all.at[pl.ds(token_row, TOKENS)], 1),
        )
        near = (
            (query.at[:, wide], query_all.at[pl.ds(side_row, TOKENS)], 2),
            (grad.at[:, wide], grad_all.at[pl.ds(side_row, TOKENS)], 3),
            (stat.at[slot], stat_all.at[side_slot], 4),
        )
        return far, near

    def send(piece, to_group, to_member):
        source, target, which = piece
        pltpu.make_async_remote_copy(
            src_ref=source,
            dst_ref=target,
            send_sem=send_sem.at[which],
            recv_sem=recv_sem.at[which],
            device_id=(to_group, to_member),
            device_id_type=MESH,
        ).start()

    @pl.loop(1, everyone)
    def _(apart):
        to_group = lax.rem(group + apart // members, groups)
        to_member = lax.rem(member + lax.rem(apart, members), members)
        slot = to_group * half + lax.rem(to_member, half)
        far, near = pieces(slot)
        for piece in far:
            send(piece, to_group, to_member)

        @pl.when(to_member // half == side)
        def _():
            for piece in near:
                send(piece, to_group, to_member)

    far, near = pieces(side_slot)
    for source, target, which in far + near:
        pltpu.make_async_copy(source, target, recv_sem.at[which]).start()
    others = (everyone - 1) * TOKENS
    near_others = (groups * half - 1) * TOKENS
    wait_bytes(key_all.at[pl.ds(0, others)], send_sem.at[0])
    wait_bytes(value_all.at[pl.ds(0, others)], send_sem.at[1])
    wait_bytes(query_all.at[pl.ds(0, near_others)], send_sem.at[2])
    wait_bytes(grad_all.at[pl.ds(0, near_others)], send_sem.at[3])
    wait_bytes(stat_all.at[pl.ds(0, groups * half - 1)], send_sem.at[4])
    for which, ref in enumerate((key_all, value_all, query_all, grad_all, stat_all)):
        wait_bytes(ref, recv_sem.at[which])


def collect_kernel(
    groups,
    members,
    grad_q,
    grad_k,
    grad_v,
    query_out,
    key_out,
    value_out,
    send_sem,
    recv_sem,
):
    half = members // 2
    everyone = groups * members
    group = lax.axis_index("seq")
    member = lax.axis_index("head")
    side = member // half
    greet_all(groups, members, group, member)
    my_slot = group * half + lax.rem(member, half)
    narrow = pl.ds(pl.multiple_of(my_slot * HEAD_SIZE, HEAD_SIZE), HEAD_SIZE)
    wide = pl.ds(pl.multiple_of(my_slot * 2 * HEAD_SIZE, 2 * HEAD_SIZE), 2 * HEAD_SIZE)

    def pieces(to_group, to_member):
        row = pl.multiple_of((to_group * members + to_member) * TOKENS, TOKENS)
        side_row = pl.multiple_of((to_group * half + lax.rem(to_member, half)) * TOKENS, TOKENS)
        return (
            (grad_k.at[pl.ds(row, TOKENS)], key_out.at[side, :, narrow], 0),
            (grad_v.at[pl.ds(row, TOKENS)], value_out.at[side, :, narrow], 1),
            (grad_q.at[pl.ds(side_row, TOKENS)], query_out.at[:, wide], 2),
        )

    def send(piece, to_group, to_member):
        source, target, which = piece
        pltpu.make_async_remote_copy(
            src_ref=source,
            dst_ref=target,
            send_sem=send_sem.at[which],
            recv_sem=recv_sem.at[which],
            device_id=(to_group, to_member),
            device_id_type=MESH,
        ).start()

    @pl.loop(1, everyone)
    def _(apart):
        to_group = lax.rem(group + apart // members, groups)
        to_member = lax.rem(member + lax.rem(apart, members), members)
        of_key, of_value, of_query = pieces(to_group, to_member)
        send(of_key, to_group, to_member)
        send(of_value, to_group, to_member)

        @pl.when(to_member // half == side)
        def _():
            send(of_query, to_group, to_member)

    for source, target, which in pieces(group, member):
        pltpu.make_async_copy(source, target, recv_sem.at[which]).start()
    others = (everyone - 1) * TOKENS
    near_others = (groups * half - 1) * TOKENS
    wait_bytes(grad_k.at[pl.ds(0, others)], send_sem.at[0])
    wait_bytes(grad_v.at[pl.ds(0, others)], send_sem.at[1])
    wait_bytes(grad_q.at[pl.ds(0, near_others)], send_sem.at[2])
    wait_bytes(key_out, recv_sem.at[0])
    wait_bytes(value_out, recv_sem.at[1])
    wait_bytes(query_out, recv_sem.at[2])


def dot(left, right, dims):
    return lax.dot_general(left, right, (dims, ((), ())), preferred_element_type=jnp.float32)


def attention_kernel(
    span,
    inner,
    scalars,
    query_all,
    grad_all,
    key_all,
    value_all,
    stat_all,
    grad_q,
    grad_k,
    grad_v,
    key_turned,
    sum_q,
    sum_k,
    sum_v,
):
    side = scalars[inner]
    per_span = span // 2 // TILE
    blocks = key_all.shape[0] // TILE

    @pl.loop(0, blocks)
    def _(block):
        rows = pl.ds(block * TILE, TILE)
        key_turned[block] = key_all[rows].T
        sum_k[rows] = jnp.zeros((TILE, HEAD_SIZE), jnp.float32)
        sum_v[rows] = jnp.zeros((TILE, HEAD_SIZE), jnp.float32)

    @pl.loop(0, query_all.shape[0] // TILE)
    def _(tile):
        first = (tile // per_span) * span + side * (span // 2) + lax.rem(tile, per_span) * TILE
        rows = pl.ds(tile * TILE, TILE)
        query = jnp.concatenate([query_all[rows, :HEAD_SIZE], query_all[rows, HEAD_SIZE:]], 0)
        grad = jnp.concatenate([grad_all[rows, :HEAD_SIZE], grad_all[rows, HEAD_SIZE:]], 0)
        parts = TILE // TOKENS
        stat = [stat_all[tile * parts + part] for part in range(parts)]
        norm = jnp.concatenate([s[h : h + 1] for h in (0, 1) for s in stat], 1)
        delta = jnp.concatenate([s[h : h + 1] for h in (2, 3) for s in stat], 1)
        spot = first + lax.rem(lax.broadcasted_iota(jnp.int32, (1, 2 * TILE), 1), TILE)
        begin = jnp.zeros((1, 2 * TILE), jnp.int32)
        lowest = jnp.int32(0)
        for cut in range(inner):
            bound = scalars[cut]
            begin = jnp.where(spot >= bound, bound, begin)
            lowest = jnp.where(first >= bound, bound, lowest)
        sum_q[...] = jnp.zeros_like(sum_q)

        @pl.loop(lowest // TILE, first // TILE + 1)
        def _(block):
            cols = pl.ds(pl.multiple_of(block * TILE, TILE), TILE)
            score = dot(key_all[cols], query, ((1,), (1,)))
            where = block * TILE + lax.broadcasted_iota(jnp.int32, (TILE, 2 * TILE), 0)
            allowed = (where >= begin) & (where <= spot)
            prob = jnp.where(allowed, jnp.exp2(score * (attn_scale * math.log2(math.e)) - norm), 0.0)
            dprob = dot(value_all[cols], grad, ((1,), (1,)))
            dscore = (prob * (dprob - delta)).astype(jnp.bfloat16)
            sum_v[cols] += dot(prob.astype(jnp.bfloat16), grad, ((1,), (0,)))
            sum_k[cols] += dot(dscore, query, ((1,), (0,)))
            sum_q[...] += dot(key_turned[block], dscore, ((1,), (0,)))

        for head in (0, 1):
            turned = (sum_q[:, head * TILE : (head + 1) * TILE] * attn_scale).T
            grad_q[rows, head * HEAD_SIZE : (head + 1) * HEAD_SIZE] = turned.astype(jnp.bfloat16)

    @pl.loop(0, blocks)
    def _(block):
        rows = pl.ds(block * TILE, TILE)
        grad_k[rows] = (sum_k[rows] * attn_scale).astype(jnp.bfloat16)
        grad_v[rows] = sum_v[rows].astype(jnp.bfloat16)


def half_shards(
    groups, members, query, key_matrix, value_matrix, output_gradient, attn_out, doc_offsets, stats
):
    half = members // 2
    slots = groups * half
    token_count = groups * members * TOKENS
    low, wide = jnp.bfloat16, jnp.float32
    delta = jnp.sum(
        (output_gradient.astype(wide) * attn_out.astype(wide)).reshape(TOKENS, HQ, HEAD_SIZE),
        axis=2,
    )
    norm = stats * math.log2(math.e)
    stat = jnp.concatenate(
        [
            norm.T.reshape(slots, 2, TOKENS),
            delta.T.reshape(slots, 2, TOKENS),
            jnp.zeros((slots, 4, TOKENS), wide),
        ],
        1,
    )
    anywhere = pl.BlockSpec(memory_space=pl.ANY)
    near_rows = slots * TOKENS
    spread = pl.pallas_call(
        functools.partial(spread_kernel, groups, members),
        out_shape=(
            jax.ShapeDtypeStruct((near_rows, 2 * HEAD_SIZE), low),
            jax.ShapeDtypeStruct((near_rows, 2 * HEAD_SIZE), low),
            jax.ShapeDtypeStruct((token_count, HEAD_SIZE), low),
            jax.ShapeDtypeStruct((token_count, HEAD_SIZE), low),
            jax.ShapeDtypeStruct((slots, 8, TOKENS), wide),
        ),
        in_specs=[anywhere] * 5,
        out_specs=[anywhere] * 5,
        scratch_shapes=[pltpu.SemaphoreType.DMA((5,)), pltpu.SemaphoreType.DMA((5,))],
        compiler_params=pltpu.CompilerParams(collective_id=0, has_side_effects=True),
        name="spread",
    )(query, output_gradient, key_matrix, value_matrix, stat)
    inner = doc_offsets.shape[0] - 2
    side = lax.axis_index("head") // half
    scalars = jnp.concatenate([doc_offsets[1:-1], side.astype(jnp.int32)[None]])
    in_vmem = pl.BlockSpec(memory_space=pltpu.VMEM)
    grad_q, grad_k, grad_v = pl.pallas_call(
        functools.partial(attention_kernel, members * TOKENS, inner),
        out_shape=(
            jax.ShapeDtypeStruct((near_rows, 2 * HEAD_SIZE), low),
            jax.ShapeDtypeStruct((token_count, HEAD_SIZE), low),
            jax.ShapeDtypeStruct((token_count, HEAD_SIZE), low),
        ),
        in_specs=[pl.BlockSpec(memory_space=pltpu.SMEM)] + [in_vmem] * 5,
        out_specs=[in_vmem] * 3,
        scratch_shapes=[
            pltpu.VMEM((token_count // TILE, HEAD_SIZE, TILE), low),
            pltpu.VMEM((HEAD_SIZE, 2 * TILE), wide),
            pltpu.VMEM((token_count, HEAD_SIZE), wide),
            pltpu.VMEM((token_count, HEAD_SIZE), wide),
        ],
        compiler_params=pltpu.CompilerParams(vmem_limit_bytes=40 * 1024 * 1024),
        name="attention",
    )(scalars, *spread)
    grad_query, key_halves, value_halves = pl.pallas_call(
        functools.partial(collect_kernel, groups, members),
        out_shape=(
            jax.ShapeDtypeStruct((TOKENS, HQ * HEAD_SIZE), low),
            jax.ShapeDtypeStruct((2, TOKENS, slots * HEAD_SIZE), low),
            jax.ShapeDtypeStruct((2, TOKENS, slots * HEAD_SIZE), low),
        ),
        in_specs=[anywhere] * 3,
        out_specs=[anywhere] * 3,
        scratch_shapes=[pltpu.SemaphoreType.DMA((3,)), pltpu.SemaphoreType.DMA((3,))],
        compiler_params=pltpu.CompilerParams(collective_id=1, has_side_effects=True),
        name="collect",
    )(grad_q, grad_k, grad_v)
    key_gradient = (key_halves[0].astype(wide) + key_halves[1].astype(wide)).astype(low)
    value_gradient = (value_halves[0].astype(wide) + value_halves[1].astype(wide)).astype(low)
    return (grad_query, key_gradient, value_gradient)


def solution(mesh):
    placed = (
        P(("seq", "head"), None),
        P(("seq", "head"), None),
        P(("seq", "head"), None),
        P(("seq", "head"), None),
        P(("seq", "head"), None),
        P(),
        P(("seq", "head"), None),
    )
    groups, members = mesh.shape["seq"], mesh.shape["head"]
    halves_fit = members % 2 == 0 and groups * (members // 2) * 2 == HQ

    def whole(*arrays):
        tokens = arrays[0].shape[0] // (groups * members)
        fits = halves_fit and tokens == TOKENS and tokens * members == 2 * DOCHALF
        body = functools.partial(half_shards, groups, members) if fits else shards
        return mapped(body)(*arrays)

    def mapped(body):
        return jax.shard_map(
            body,
            mesh=mesh,
            in_specs=placed,
            out_specs=(P(("seq", "head"), None), P(("seq", "head"), None), P(("seq", "head"), None)),
            check_vma=False,
        )

    return whole
```

```python
import functools
import math

import jax
import jax.numpy as jnp
from jax import lax
from jax.experimental import pallas as pl
from jax.experimental.pallas import tpu as pltpu
from jax.sharding import PartitionSpec as P

HQ = 32
HEAD_SIZE = 128
DOCHALF = 512
QBLK = 512


attn_scale = 144.0 ** (-0.5)


def partner(value, axis, apart):
    mask = 2**apart
    pairs = [(source, source ^ mask) for source in range(lax.axis_size(axis))]
    return lax.ppermute(value, axis, pairs)


def from_behind(value, axis, steps):
    count = lax.axis_size(axis)
    leading, last = (max(0, -steps), min(count, count - steps))
    return lax.ppermute(value, axis, [(source, source + steps) for source in range(leading, last)])


def tile_grads(query_rows, grad_rows, lse_rows, delta_rows, key_window, value_window, allowed):
    score = (
        jnp.einsum("qgrd,kgd->grqk", query_rows, key_window, preferred_element_type=jnp.float32)
        * attn_scale
    )
    norm_stat = jnp.transpose(lse_rows, (1, 2, 0))[..., None]
    prob = jnp.where(allowed[None, None], jnp.exp(score - norm_stat), 0.0)
    dprob = jnp.einsum(
        "qgrd,kgd->grqk", grad_rows, value_window, preferred_element_type=jnp.float32
    )
    dscore = prob * (dprob - jnp.transpose(delta_rows, (1, 2, 0))[..., None])
    prob_low = prob.astype(jnp.bfloat16)
    dscore_low = dscore.astype(jnp.bfloat16)
    value_gradient = jnp.einsum(
        "grqk,qgrd->kgd", prob_low, grad_rows, preferred_element_type=jnp.float32
    )
    key_gradient = (
        jnp.einsum("grqk,qgrd->kgd", dscore_low, query_rows, preferred_element_type=jnp.float32)
        * attn_scale
    )
    grad_query = (
        jnp.einsum("grqk,kgd->qgrd", dscore_low, key_window, preferred_element_type=jnp.float32)
        * attn_scale
    )
    return (grad_query, key_gradient, value_gradient)


def doc_numbers(positions, inner):
    return jnp.sum((inner[None, :] <= positions[:, None]).astype(jnp.int32), axis=1)


def shards(query, key_matrix, value_matrix, output_gradient, attn_out, doc_offsets, stats):
    token_count_local = query.shape[0]
    members = lax.axis_size("head")
    group_span = token_count_local * members
    per_device = HQ // members
    lookback = 2 * DOCHALF
    width = lookback + QBLK
    group = lax.axis_index("seq")
    member = lax.axis_index("head")
    parity = member % 2
    half_width = HEAD_SIZE // 2
    delta_correction = jnp.sum(
        (output_gradient.astype(jnp.float32) * attn_out.astype(jnp.float32)).reshape(
            token_count_local, HQ, HEAD_SIZE
        ),
        axis=2,
    )
    query_heads, grad_heads = (
        lax.all_to_all(query, "head", split_axis=1, concat_axis=0, tiled=True),
        lax.all_to_all(output_gradient, "head", split_axis=1, concat_axis=0, tiled=True),
    )
    lse_heads, delta_heads = (
        lax.all_to_all(stats, "head", split_axis=1, concat_axis=0, tiled=True),
        lax.all_to_all(delta_correction, "head", split_axis=1, concat_axis=0, tiled=True),
    )
    key_cols, value_cols = (
        lax.all_to_all(key_matrix, "head", split_axis=1, concat_axis=0, tiled=True),
        lax.all_to_all(value_matrix, "head", split_axis=1, concat_axis=0, tiled=True),
    )
    if per_device >= 2:
        groups = per_device // 2
        key_heads = key_cols.reshape(group_span, groups, HEAD_SIZE)
        value_heads = value_cols.reshape(group_span, groups, HEAD_SIZE)
    else:
        groups = 1
        other_key, other_value = partner((key_cols, value_cols), "head", 0)
        key_heads = jnp.where(
            parity == 0,
            jnp.concatenate([key_cols, other_key], 1),
            jnp.concatenate([other_key, key_cols], 1),
        ).reshape(group_span, 1, HEAD_SIZE)
        value_heads = jnp.where(
            parity == 0,
            jnp.concatenate([value_cols, other_value], 1),
            jnp.concatenate([other_value, value_cols], 1),
        ).reshape(group_span, 1, HEAD_SIZE)
    repeats = per_device // groups
    query_heads = query_heads.reshape(group_span, groups, repeats, HEAD_SIZE)
    grad_heads = grad_heads.reshape(group_span, groups, repeats, HEAD_SIZE)
    lse_heads = lse_heads.reshape(group_span, groups, repeats)
    delta_heads = delta_heads.reshape(group_span, groups, repeats)
    prior_key, prior_value = from_behind(
        (key_heads[group_span - lookback :], value_heads[group_span - lookback :]), "seq", 1
    )
    key_ext = jnp.concatenate([prior_key, key_heads], 0)
    value_ext = jnp.concatenate([prior_value, value_heads], 0)
    inner = doc_offsets[1:-1]
    query_pos = group * group_span + jnp.arange(group_span, dtype=jnp.int32)
    key_pos = group * group_span - lookback + jnp.arange(lookback + group_span, dtype=jnp.int32)
    query_doc = doc_numbers(query_pos, inner)
    key_doc = doc_numbers(key_pos, inner)

    def block_step(block, carry):
        grad_q, grad_k, grad_v = carry
        start = (block * QBLK).astype(jnp.int32)
        query_rows = lax.dynamic_slice_in_dim(query_heads, start, QBLK, 0)
        grad_rows = lax.dynamic_slice_in_dim(grad_heads, start, QBLK, 0)
        lse_rows = lax.dynamic_slice_in_dim(lse_heads, start, QBLK, 0)
        delta_rows = lax.dynamic_slice_in_dim(delta_heads, start, QBLK, 0)
        key_window = lax.dynamic_slice_in_dim(key_ext, start, width, 0)
        value_window = lax.dynamic_slice_in_dim(value_ext, start, width, 0)
        rows_pos = lax.dynamic_slice_in_dim(query_pos, start, QBLK, 0)
        rows_doc = lax.dynamic_slice_in_dim(query_doc, start, QBLK, 0)
        cols_pos = lax.dynamic_slice_in_dim(key_pos, start, width, 0)
        cols_doc = lax.dynamic_slice_in_dim(key_doc, start, width, 0)
        allowed = (
            (cols_doc[None, :] == rows_doc[:, None])
            & (cols_pos[None, :] <= rows_pos[:, None])
            & (cols_pos[None, :] >= 0)
        )
        block_q, block_k, block_v = tile_grads(
            query_rows, grad_rows, lse_rows, delta_rows, key_window, value_window, allowed
        )
        grad_q = lax.dynamic_update_slice_in_dim(grad_q, block_q, start, 0)
        grad_k = lax.dynamic_update_slice_in_dim(
            grad_k, lax.dynamic_slice_in_dim(grad_k, start, width, 0) + block_k, start, 0
        )
        grad_v = lax.dynamic_update_slice_in_dim(
            grad_v, lax.dynamic_slice_in_dim(grad_v, start, width, 0) + block_v, start, 0
        )
        return (grad_q, grad_k, grad_v)

    init = (
        jnp.zeros((group_span, groups, repeats, HEAD_SIZE), jnp.float32),
        jnp.zeros((lookback + group_span, groups, HEAD_SIZE), jnp.float32),
        jnp.zeros((lookback + group_span, groups, HEAD_SIZE), jnp.float32),
    )
    grad_q, grad_k, grad_v = lax.fori_loop(0, group_span // QBLK, block_step, init)
    back_key, back_value = (
        from_behind(grad_k[:lookback].astype(jnp.bfloat16), "seq", -1).astype(jnp.float32),
        from_behind(grad_v[:lookback].astype(jnp.bfloat16), "seq", -1).astype(jnp.float32),
    )
    own_key = grad_k[lookback:].at[group_span - lookback :].add(back_key)
    own_value = grad_v[lookback:].at[group_span - lookback :].add(back_value)
    query_low = grad_q.astype(jnp.bfloat16).reshape(group_span, per_device * HEAD_SIZE)
    grad_query = lax.all_to_all(query_low, "head", split_axis=0, concat_axis=1, tiled=True)
    if per_device >= 2:
        send_key = own_key.reshape(group_span, groups * HEAD_SIZE)
        send_value = own_value.reshape(group_span, groups * HEAD_SIZE)
    else:
        flat_key = own_key.reshape(group_span, HEAD_SIZE)
        flat_value = own_value.reshape(group_span, HEAD_SIZE)
        keep_key = lax.dynamic_slice_in_dim(flat_key, parity * half_width, half_width, 1)
        keep_value = lax.dynamic_slice_in_dim(flat_value, parity * half_width, half_width, 1)
        give_key = lax.dynamic_slice_in_dim(flat_key, (1 - parity) * half_width, half_width, 1)
        give_value = lax.dynamic_slice_in_dim(flat_value, (1 - parity) * half_width, half_width, 1)
        from_key, from_value = partner((give_key, give_value), "head", 0)
        send_key = keep_key + from_key
        send_value = keep_value + from_value
    key_gradient_summed, value_gradient_summed = (
        lax.all_to_all(
            send_key.astype(jnp.bfloat16), "head", split_axis=0, concat_axis=1, tiled=True
        ).astype(send_key.dtype),
        lax.all_to_all(
            send_value.astype(jnp.bfloat16), "head", split_axis=0, concat_axis=1, tiled=True
        ).astype(send_value.dtype),
    )
    key_gradient = key_gradient_summed.astype(jnp.bfloat16)
    value_gradient = value_gradient_summed.astype(jnp.bfloat16)
    return (grad_query, key_gradient, value_gradient)


TOKENS = 128
TILE = 256
PHASE = 8
MESH = pl.DeviceIdType.MESH


def wait_bytes(ref, sem):
    pltpu.make_async_copy(ref, ref, sem).wait()


def greet_all(groups, members, group, member):
    barrier = pltpu.get_barrier_semaphore()
    everyone = groups * members

    @pl.loop(1, everyone)
    def _(apart):
        to_group = lax.rem(group + apart // members, groups)
        to_member = lax.rem(member + lax.rem(apart, members), members)
        pl.semaphore_signal(barrier, inc=1, device_id=(to_group, to_member), device_id_type=MESH)

    pl.semaphore_wait(barrier, everyone - 1)


def fused_kernel(
    groups,
    members,
    inner,
    offsets,
    query,
    grad,
    key,
    value,
    attn_out,
    norm,
    query_out,
    key_out,
    value_out,
    query_all,
    grad_all,
    key_all,
    value_all,
    stat_all,
    grad_own,
    out_own,
    stat_own,
    grad_q,
    grad_k,
    grad_v,
    key_turned,
    sum_q,
    sum_k,
    sum_v,
    send_sem,
    recv_sem,
    own_sem,
):
    half = members // 2
    everyone = groups * members
    group = lax.axis_index("seq")
    member = lax.axis_index("head")
    side = member // half
    greet_all(groups, members, group, member)
    token_row = pl.multiple_of((group * members + member) * TOKENS, TOKENS)
    side_slot = group * half + lax.rem(member, half)
    side_row = pl.multiple_of(side_slot * TOKENS, TOKENS)

    def pieces(slot):
        narrow = pl.ds(pl.multiple_of(slot * HEAD_SIZE, HEAD_SIZE), HEAD_SIZE)
        wide = pl.ds(pl.multiple_of(slot * 2 * HEAD_SIZE, 2 * HEAD_SIZE), 2 * HEAD_SIZE)
        far = (
            (key.at[:, narrow], key_all.at[pl.ds(token_row, TOKENS)], 0),
            (value.at[:, narrow], value_all.at[pl.ds(token_row, TOKENS)], 1),
        )
        near = (
            (query.at[:, wide], query_all.at[pl.ds(side_row, TOKENS)], 2),
            (grad.at[:, wide], grad_all.at[pl.ds(side_row, TOKENS)], 3),
            (stat_own.at[slot], stat_all.at[side_slot], 4),
        )
        return far, near

    def send(piece, to_group, to_member):
        source, target, which = piece
        pltpu.make_async_remote_copy(
            src_ref=source,
            dst_ref=target,
            send_sem=send_sem.at[which],
            recv_sem=recv_sem.at[which],
            device_id=(to_group, to_member),
            device_id_type=MESH,
        ).start()

    @pl.loop(0, groups * half)
    def _(step):
        turn = lax.rem(step + lax.rem(group, 2) * PHASE, groups * half)
        to_group = lax.rem(group + turn // half, groups)
        to_local = lax.rem(member + lax.rem(turn, half), half)
        slot = to_group * half + to_local
        far, near = pieces(slot)
        here = (to_group, side * half + to_local)
        across = (to_group, (1 - side) * half + to_local)

        @pl.when(turn > 0)
        def _():
            send(far[0], *here)
            send(far[1], *here)

        send(far[0], *across)

        @pl.when(turn > 0)
        def _():
            send(near[0], *here)

        send(far[1], *across)

        @pl.when(turn > 0)
        def _():
            send(near[1], *here)

    load_grad = pltpu.make_async_copy(grad, grad_own, own_sem.at[0])
    load_out = pltpu.make_async_copy(attn_out, out_own, own_sem.at[1])
    load_grad.start()
    load_out.start()
    load_grad.wait()
    load_out.wait()
    for slot in range(groups * half):
        for part in range(2):
            head = 2 * slot + part
            columns = slice(head * HEAD_SIZE, (head + 1) * HEAD_SIZE)
            both = grad_own[:, columns].astype(jnp.float32) * out_own[:, columns].astype(jnp.float32)
            stat_own[slot, 2 + part : 3 + part] = jnp.sum(both.T, axis=0, keepdims=True)
            stat_own[slot, part : part + 1] = norm[head : head + 1] * math.log2(math.e)
        stat_own[slot, 4:8] = jnp.zeros((4, TOKENS), jnp.float32)

    far, near = pieces(side_slot)
    for source, target, which in far + near[:2]:
        pltpu.make_async_copy(source, target, recv_sem.at[which]).start()
    others = (everyone - 1) * TOKENS
    near_others = (groups * half - 1) * TOKENS
    wait_bytes(key_all.at[pl.ds(0, others)], send_sem.at[0])

    @pl.loop(1, groups * half)
    def _(turn):
        to_group = lax.rem(group + turn // half, groups)
        to_local = lax.rem(member + lax.rem(turn, half), half)
        send(pieces(to_group * half + to_local)[1][2], to_group, side * half + to_local)

    pltpu.make_async_copy(stat_own.at[side_slot], stat_all.at[side_slot], recv_sem.at[4]).start()
    wait_bytes(key_all, recv_sem.at[0])

    @pl.loop(0, key_all.shape[0] // TILE)
    def _(block):
        rows = pl.ds(pl.multiple_of(block * TILE, TILE), TILE)
        key_turned[block] = key_all[rows].T
        sum_k[rows] = jnp.zeros((TILE, HEAD_SIZE), jnp.float32)
        sum_v[rows] = jnp.zeros((TILE, HEAD_SIZE), jnp.float32)

    wait_bytes(value_all, recv_sem.at[1])
    wait_bytes(query_all, recv_sem.at[2])
    wait_bytes(grad_all, recv_sem.at[3])
    wait_bytes(stat_all, recv_sem.at[4])
    span = members * TOKENS
    per_span = span // 2 // TILE
    parts = TILE // TOKENS
    narrow = pl.ds(pl.multiple_of(side_slot * HEAD_SIZE, HEAD_SIZE), HEAD_SIZE)
    wide = pl.ds(pl.multiple_of(side_slot * 2 * HEAD_SIZE, 2 * HEAD_SIZE), 2 * HEAD_SIZE)

    def compute(at_group, tile):
        first = at_group * span + side * (span // 2) + tile * TILE
        slot = at_group * half + tile * parts
        rows = pl.ds(pl.multiple_of(slot * TOKENS, TOKENS), TILE)
        queries = jnp.concatenate([query_all[rows, :HEAD_SIZE], query_all[rows, HEAD_SIZE:]], 0)
        grads = jnp.concatenate([grad_all[rows, :HEAD_SIZE], grad_all[rows, HEAD_SIZE:]], 0)
        stat = [stat_all[slot + part] for part in range(parts)]
        level = jnp.concatenate([s[h : h + 1] for h in (0, 1) for s in stat], 1)
        delta = jnp.concatenate([s[h : h + 1] for h in (2, 3) for s in stat], 1)
        spot = first + lax.rem(lax.broadcasted_iota(jnp.int32, (1, 2 * TILE), 1), TILE)
        begin = jnp.zeros((1, 2 * TILE), jnp.int32)
        for cut in range(inner):
            bound = offsets[cut + 1]
            begin = jnp.where(spot >= bound, bound, begin)
        sum_q[...] = jnp.zeros_like(sum_q)
        back_blocks = span // TILE

        @pl.loop(0, back_blocks + 1)
        def _(step):
            block = first // TILE + step - back_blocks

            @pl.when(block >= 0)
            def _():
                cols = pl.ds(pl.multiple_of(block * TILE, TILE), TILE)
                score = dot(key_all[cols], queries, ((1,), (1,)))
                where = block * TILE + lax.broadcasted_iota(jnp.int32, (TILE, 2 * TILE), 0)
                allowed = (where >= begin) & (where <= spot)
                power = jnp.exp2(score * (attn_scale * math.log2(math.e)) - level)
                prob = jnp.where(allowed, power, 0.0)
                dprob = dot(value_all[cols], grads, ((1,), (1,)))
                dscore = (prob * (dprob - delta)).astype(jnp.bfloat16)
                sum_v[cols] += dot(prob.astype(jnp.bfloat16), grads, ((1,), (0,)))
                sum_k[cols] += dot(dscore, queries, ((1,), (0,)))
                sum_q[...] += dot(key_turned[block], dscore, ((1,), (0,)))

        for part in (0, 1):
            turned = (sum_q[:, part * TILE : (part + 1) * TILE] * attn_scale).T
            grad_q[rows, part * HEAD_SIZE : (part + 1) * HEAD_SIZE] = turned.astype(jnp.bfloat16)

    def give(piece, to_group, to_member):
        mine = (to_group == group) & (to_member == member)

        @pl.when(mine)
        def _():
            source, target, which = piece
            pltpu.make_async_copy(source, target, recv_sem.at[which]).start()

        @pl.when(jnp.logical_not(mine))
        def _():
            send(piece, to_group, to_member)

    def give_query(at_group, tile):
        for part in range(parts):
            local = tile * parts + part
            row = pl.multiple_of((at_group * half + local) * TOKENS, TOKENS)
            piece = (grad_q.at[pl.ds(row, TOKENS)], query_out.at[:, wide], 5)
            give(piece, at_group, side * half + local)

    def each_owner(chunk, act):
        @pl.loop(0, members)
        def _(step):
            owner = (chunk - 1) * members + side * half + lax.rem(step + member, members)

            @pl.when((owner >= 0) & (owner < everyone))
            def _():
                act(owner, pl.ds(pl.multiple_of(owner * TOKENS, TOKENS), TOKENS))

    def settle(owner, rows):
        grad_k[rows] = (sum_k[rows] * attn_scale).astype(jnp.bfloat16)
        grad_v[rows] = sum_v[rows].astype(jnp.bfloat16)

    def give_key(owner, rows):
        to_group, to_member = owner // members, lax.rem(owner, members)
        give((grad_k.at[rows], key_out.at[side, :, narrow], 6), to_group, to_member)
        give((grad_v.at[rows], value_out.at[side, :, narrow], 7), to_group, to_member)

    def finished(turn, act):
        at_group = lax.rem(group + turn, groups)

        @pl.when((turn > 0) | (at_group == 0))
        def _():
            each_owner(at_group, act)

        @pl.when(at_group == groups - 1)
        def _():
            each_owner(groups, act)

        @pl.when((turn == groups - 1) & (group > 0))
        def _():
            each_owner(group, act)

    @pl.loop(0, groups)
    def _(turn):
        at_group = lax.rem(group + turn, groups)

        @pl.loop(0, per_span)
        def _(part):
            tile = lax.rem(part + lax.rem(member, half) // 2, per_span)
            compute(at_group, tile)

            @pl.when(part > 0)
            def _():
                give_query(at_group, lax.rem(tile + per_span - 1, per_span))

            @pl.when((part == 0) & (turn > 0))
            def _():
                finished(turn - 1, give_key)

        finished(turn, settle)
        last = lax.rem(per_span - 1 + lax.rem(member, half) // 2, per_span)
        give_query(at_group, last)

    finished(groups - 1, give_key)
    wait_bytes(value_all.at[pl.ds(0, others)], send_sem.at[1])
    wait_bytes(query_all.at[pl.ds(0, near_others)], send_sem.at[2])
    wait_bytes(grad_all.at[pl.ds(0, near_others)], send_sem.at[3])
    wait_bytes(stat_all.at[pl.ds(0, groups * half - 1)], send_sem.at[4])
    wait_bytes(grad_q.at[pl.ds(0, near_others)], send_sem.at[5])
    wait_bytes(grad_k.at[pl.ds(0, others)], send_sem.at[6])
    wait_bytes(grad_v.at[pl.ds(0, others)], send_sem.at[7])
    wait_bytes(query_out, recv_sem.at[5])
    wait_bytes(key_out, recv_sem.at[6])
    wait_bytes(value_out, recv_sem.at[7])


def dot(left, right, dims):
    return lax.dot_general(left, right, (dims, ((), ())), preferred_element_type=jnp.float32)


def half_shards(
    groups, members, query, key_matrix, value_matrix, output_gradient, attn_out, doc_offsets, stats
):
    slots = groups * (members // 2)
    token_count = groups * members * TOKENS
    near_rows = slots * TOKENS
    low, wide = jnp.bfloat16, jnp.float32
    in_vmem = pl.BlockSpec(memory_space=pltpu.VMEM)
    in_smem = pl.BlockSpec(memory_space=pltpu.SMEM)
    anywhere = pl.BlockSpec(memory_space=pl.ANY)
    grad_query, key_halves, value_halves = pl.pallas_call(
        functools.partial(fused_kernel, groups, members, doc_offsets.shape[0] - 2),
        out_shape=(
            jax.ShapeDtypeStruct((TOKENS, HQ * HEAD_SIZE), low),
            jax.ShapeDtypeStruct((2, TOKENS, slots * HEAD_SIZE), low),
            jax.ShapeDtypeStruct((2, TOKENS, slots * HEAD_SIZE), low),
        ),
        in_specs=[in_smem] + [anywhere] * 5 + [in_vmem],
        out_specs=[anywhere] * 3,
        scratch_shapes=[
            pltpu.VMEM((near_rows, 2 * HEAD_SIZE), low),
            pltpu.VMEM((near_rows, 2 * HEAD_SIZE), low),
            pltpu.VMEM((token_count, HEAD_SIZE), low),
            pltpu.VMEM((token_count, HEAD_SIZE), low),
            pltpu.VMEM((slots, 8, TOKENS), wide),
            pltpu.VMEM((TOKENS, HQ * HEAD_SIZE), low),
            pltpu.VMEM((TOKENS, HQ * HEAD_SIZE), low),
            pltpu.VMEM((slots, 8, TOKENS), wide),
            pltpu.VMEM((near_rows, 2 * HEAD_SIZE), low),
            pltpu.VMEM((token_count, HEAD_SIZE), low),
            pltpu.VMEM((token_count, HEAD_SIZE), low),
            pltpu.VMEM((token_count // TILE, HEAD_SIZE, TILE), low),
            pltpu.VMEM((HEAD_SIZE, 2 * TILE), wide),
            pltpu.VMEM((token_count, HEAD_SIZE), wide),
            pltpu.VMEM((token_count, HEAD_SIZE), wide),
            pltpu.SemaphoreType.DMA((8,)),
            pltpu.SemaphoreType.DMA((8,)),
            pltpu.SemaphoreType.DMA((2,)),
        ],
        compiler_params=pltpu.CompilerParams(
            collective_id=0, has_side_effects=True
        ),
        name="fused",
    )(doc_offsets, query, output_gradient, key_matrix, value_matrix, attn_out, stats.T)
    key_gradient = (key_halves[0].astype(wide) + key_halves[1].astype(wide)).astype(low)
    value_gradient = (value_halves[0].astype(wide) + value_halves[1].astype(wide)).astype(low)
    return (grad_query, key_gradient, value_gradient)


def solution(mesh):
    placed = (
        P(("seq", "head"), None),
        P(("seq", "head"), None),
        P(("seq", "head"), None),
        P(("seq", "head"), None),
        P(("seq", "head"), None),
        P(),
        P(("seq", "head"), None),
    )
    groups, members = mesh.shape["seq"], mesh.shape["head"]
    halves_fit = members % 2 == 0 and groups * (members // 2) * 2 == HQ

    def whole(*arrays):
        tokens = arrays[0].shape[0] // (groups * members)
        fits = halves_fit and tokens == TOKENS and tokens * members == 2 * DOCHALF
        body = functools.partial(half_shards, groups, members) if fits else shards
        return mapped(body)(*arrays)

    def mapped(body):
        return jax.shard_map(
            body,
            mesh=mesh,
            in_specs=placed,
            out_specs=(P(("seq", "head"), None), P(("seq", "head"), None), P(("seq", "head"), None)),
            check_vma=False,
        )

    return whole
```

```python
import functools
import math

import jax
import jax.numpy as jnp
from jax import lax
from jax.experimental import pallas as pl
from jax.experimental.pallas import tpu as pltpu
from jax.sharding import PartitionSpec as P

HQ = 32
HEAD_SIZE = 128
DOCHALF = 512
QBLK = 512


attn_scale = 144.0 ** (-0.5)


def partner(value, axis, apart):
    mask = 2**apart
    pairs = [(source, source ^ mask) for source in range(lax.axis_size(axis))]
    return lax.ppermute(value, axis, pairs)


def from_behind(value, axis, steps):
    count = lax.axis_size(axis)
    leading, last = (max(0, -steps), min(count, count - steps))
    return lax.ppermute(value, axis, [(source, source + steps) for source in range(leading, last)])


def tile_grads(query_rows, grad_rows, lse_rows, delta_rows, key_window, value_window, allowed):
    score = (
        jnp.einsum("qgrd,kgd->grqk", query_rows, key_window, preferred_element_type=jnp.float32)
        * attn_scale
    )
    norm_stat = jnp.transpose(lse_rows, (1, 2, 0))[..., None]
    prob = jnp.where(allowed[None, None], jnp.exp(score - norm_stat), 0.0)
    dprob = jnp.einsum(
        "qgrd,kgd->grqk", grad_rows, value_window, preferred_element_type=jnp.float32
    )
    dscore = prob * (dprob - jnp.transpose(delta_rows, (1, 2, 0))[..., None])
    prob_low = prob.astype(jnp.bfloat16)
    dscore_low = dscore.astype(jnp.bfloat16)
    value_gradient = jnp.einsum(
        "grqk,qgrd->kgd", prob_low, grad_rows, preferred_element_type=jnp.float32
    )
    key_gradient = (
        jnp.einsum("grqk,qgrd->kgd", dscore_low, query_rows, preferred_element_type=jnp.float32)
        * attn_scale
    )
    grad_query = (
        jnp.einsum("grqk,kgd->qgrd", dscore_low, key_window, preferred_element_type=jnp.float32)
        * attn_scale
    )
    return (grad_query, key_gradient, value_gradient)


def doc_numbers(positions, inner):
    return jnp.sum((inner[None, :] <= positions[:, None]).astype(jnp.int32), axis=1)


def shards(query, key_matrix, value_matrix, output_gradient, attn_out, doc_offsets, stats):
    token_count_local = query.shape[0]
    members = lax.axis_size("head")
    group_span = token_count_local * members
    per_device = HQ // members
    lookback = 2 * DOCHALF
    width = lookback + QBLK
    group = lax.axis_index("seq")
    member = lax.axis_index("head")
    parity = member % 2
    half_width = HEAD_SIZE // 2
    delta_correction = jnp.sum(
        (output_gradient.astype(jnp.float32) * attn_out.astype(jnp.float32)).reshape(
            token_count_local, HQ, HEAD_SIZE
        ),
        axis=2,
    )
    query_heads, grad_heads = (
        lax.all_to_all(query, "head", split_axis=1, concat_axis=0, tiled=True),
        lax.all_to_all(output_gradient, "head", split_axis=1, concat_axis=0, tiled=True),
    )
    lse_heads, delta_heads = (
        lax.all_to_all(stats, "head", split_axis=1, concat_axis=0, tiled=True),
        lax.all_to_all(delta_correction, "head", split_axis=1, concat_axis=0, tiled=True),
    )
    key_cols, value_cols = (
        lax.all_to_all(key_matrix, "head", split_axis=1, concat_axis=0, tiled=True),
        lax.all_to_all(value_matrix, "head", split_axis=1, concat_axis=0, tiled=True),
    )
    if per_device >= 2:
        groups = per_device // 2
        key_heads = key_cols.reshape(group_span, groups, HEAD_SIZE)
        value_heads = value_cols.reshape(group_span, groups, HEAD_SIZE)
    else:
        groups = 1
        other_key, other_value = partner((key_cols, value_cols), "head", 0)
        key_heads = jnp.where(
            parity == 0,
            jnp.concatenate([key_cols, other_key], 1),
            jnp.concatenate([other_key, key_cols], 1),
        ).reshape(group_span, 1, HEAD_SIZE)
        value_heads = jnp.where(
            parity == 0,
            jnp.concatenate([value_cols, other_value], 1),
            jnp.concatenate([other_value, value_cols], 1),
        ).reshape(group_span, 1, HEAD_SIZE)
    repeats = per_device // groups
    query_heads = query_heads.reshape(group_span, groups, repeats, HEAD_SIZE)
    grad_heads = grad_heads.reshape(group_span, groups, repeats, HEAD_SIZE)
    lse_heads = lse_heads.reshape(group_span, groups, repeats)
    delta_heads = delta_heads.reshape(group_span, groups, repeats)
    prior_key, prior_value = from_behind(
        (key_heads[group_span - lookback :], value_heads[group_span - lookback :]), "seq", 1
    )
    key_ext = jnp.concatenate([prior_key, key_heads], 0)
    value_ext = jnp.concatenate([prior_value, value_heads], 0)
    inner = doc_offsets[1:-1]
    query_pos = group * group_span + jnp.arange(group_span, dtype=jnp.int32)
    key_pos = group * group_span - lookback + jnp.arange(lookback + group_span, dtype=jnp.int32)
    query_doc = doc_numbers(query_pos, inner)
    key_doc = doc_numbers(key_pos, inner)

    def block_step(block, carry):
        grad_q, grad_k, grad_v = carry
        start = (block * QBLK).astype(jnp.int32)
        query_rows = lax.dynamic_slice_in_dim(query_heads, start, QBLK, 0)
        grad_rows = lax.dynamic_slice_in_dim(grad_heads, start, QBLK, 0)
        lse_rows = lax.dynamic_slice_in_dim(lse_heads, start, QBLK, 0)
        delta_rows = lax.dynamic_slice_in_dim(delta_heads, start, QBLK, 0)
        key_window = lax.dynamic_slice_in_dim(key_ext, start, width, 0)
        value_window = lax.dynamic_slice_in_dim(value_ext, start, width, 0)
        rows_pos = lax.dynamic_slice_in_dim(query_pos, start, QBLK, 0)
        rows_doc = lax.dynamic_slice_in_dim(query_doc, start, QBLK, 0)
        cols_pos = lax.dynamic_slice_in_dim(key_pos, start, width, 0)
        cols_doc = lax.dynamic_slice_in_dim(key_doc, start, width, 0)
        allowed = (
            (cols_doc[None, :] == rows_doc[:, None])
            & (cols_pos[None, :] <= rows_pos[:, None])
            & (cols_pos[None, :] >= 0)
        )
        block_q, block_k, block_v = tile_grads(
            query_rows, grad_rows, lse_rows, delta_rows, key_window, value_window, allowed
        )
        grad_q = lax.dynamic_update_slice_in_dim(grad_q, block_q, start, 0)
        grad_k = lax.dynamic_update_slice_in_dim(
            grad_k, lax.dynamic_slice_in_dim(grad_k, start, width, 0) + block_k, start, 0
        )
        grad_v = lax.dynamic_update_slice_in_dim(
            grad_v, lax.dynamic_slice_in_dim(grad_v, start, width, 0) + block_v, start, 0
        )
        return (grad_q, grad_k, grad_v)

    init = (
        jnp.zeros((group_span, groups, repeats, HEAD_SIZE), jnp.float32),
        jnp.zeros((lookback + group_span, groups, HEAD_SIZE), jnp.float32),
        jnp.zeros((lookback + group_span, groups, HEAD_SIZE), jnp.float32),
    )
    grad_q, grad_k, grad_v = lax.fori_loop(0, group_span // QBLK, block_step, init)
    back_key, back_value = (
        from_behind(grad_k[:lookback].astype(jnp.bfloat16), "seq", -1).astype(jnp.float32),
        from_behind(grad_v[:lookback].astype(jnp.bfloat16), "seq", -1).astype(jnp.float32),
    )
    own_key = grad_k[lookback:].at[group_span - lookback :].add(back_key)
    own_value = grad_v[lookback:].at[group_span - lookback :].add(back_value)
    query_low = grad_q.astype(jnp.bfloat16).reshape(group_span, per_device * HEAD_SIZE)
    grad_query = lax.all_to_all(query_low, "head", split_axis=0, concat_axis=1, tiled=True)
    if per_device >= 2:
        send_key = own_key.reshape(group_span, groups * HEAD_SIZE)
        send_value = own_value.reshape(group_span, groups * HEAD_SIZE)
    else:
        flat_key = own_key.reshape(group_span, HEAD_SIZE)
        flat_value = own_value.reshape(group_span, HEAD_SIZE)
        keep_key = lax.dynamic_slice_in_dim(flat_key, parity * half_width, half_width, 1)
        keep_value = lax.dynamic_slice_in_dim(flat_value, parity * half_width, half_width, 1)
        give_key = lax.dynamic_slice_in_dim(flat_key, (1 - parity) * half_width, half_width, 1)
        give_value = lax.dynamic_slice_in_dim(flat_value, (1 - parity) * half_width, half_width, 1)
        from_key, from_value = partner((give_key, give_value), "head", 0)
        send_key = keep_key + from_key
        send_value = keep_value + from_value
    key_gradient_summed, value_gradient_summed = (
        lax.all_to_all(
            send_key.astype(jnp.bfloat16), "head", split_axis=0, concat_axis=1, tiled=True
        ).astype(send_key.dtype),
        lax.all_to_all(
            send_value.astype(jnp.bfloat16), "head", split_axis=0, concat_axis=1, tiled=True
        ).astype(send_value.dtype),
    )
    key_gradient = key_gradient_summed.astype(jnp.bfloat16)
    value_gradient = value_gradient_summed.astype(jnp.bfloat16)
    return (grad_query, key_gradient, value_gradient)


TOKENS = 128
TILE = 256
MESH = pl.DeviceIdType.MESH


def wait_bytes(ref, sem):
    pltpu.make_async_copy(ref, ref, sem).wait()


def greet_all(groups, members, group, member):
    barrier = pltpu.get_barrier_semaphore()
    everyone = groups * members

    @pl.loop(1, everyone)
    def _(apart):
        to_group = lax.rem(group + apart // members, groups)
        to_member = lax.rem(member + lax.rem(apart, members), members)
        pl.semaphore_signal(barrier, inc=1, device_id=(to_group, to_member), device_id_type=MESH)

    pl.semaphore_wait(barrier, everyone - 1)


def fused_kernel(
    groups,
    members,
    inner,
    offsets,
    query,
    grad,
    key,
    value,
    attn_out,
    norm,
    query_out,
    key_out,
    value_out,
    query_all,
    grad_all,
    key_all,
    value_all,
    stat_all,
    grad_own,
    out_own,
    stat_own,
    grad_q,
    grad_k,
    grad_v,
    key_turned,
    sum_q,
    sum_k,
    sum_v,
    send_sem,
    recv_sem,
    own_sem,
):
    half = members // 2
    everyone = groups * members
    group = lax.axis_index("seq")
    member = lax.axis_index("head")
    side = member // half
    greet_all(groups, members, group, member)
    token_row = pl.multiple_of((group * members + member) * TOKENS, TOKENS)
    side_slot = group * half + lax.rem(member, half)
    side_row = pl.multiple_of(side_slot * TOKENS, TOKENS)

    def pieces(slot):
        narrow = pl.ds(pl.multiple_of(slot * HEAD_SIZE, HEAD_SIZE), HEAD_SIZE)
        wide = pl.ds(pl.multiple_of(slot * 2 * HEAD_SIZE, 2 * HEAD_SIZE), 2 * HEAD_SIZE)
        far = (
            (key.at[:, narrow], key_all.at[pl.ds(token_row, TOKENS)], 0),
            (value.at[:, narrow], value_all.at[pl.ds(token_row, TOKENS)], 1),
        )
        near = (
            (query.at[:, wide], query_all.at[pl.ds(side_row, TOKENS)], 2),
            (grad.at[:, wide], grad_all.at[pl.ds(side_row, TOKENS)], 3),
            (stat_own.at[slot], stat_all.at[side_slot], 4),
        )
        return far, near

    def slot_of(which):
        return group if which < 5 else 0

    def send(piece, to_group, to_member):
        source, target, which = piece
        pltpu.make_async_remote_copy(
            src_ref=source,
            dst_ref=target,
            send_sem=send_sem.at[which],
            recv_sem=recv_sem.at[which, slot_of(which)],
            device_id=(to_group, to_member),
            device_id_type=MESH,
        ).start()

    def send_group(apart, keys, queries):
        to_group = lax.rem(group + apart, groups)

        @pl.loop(0, half)
        def _(step):
            to_local = lax.rem(member + step, half)
            far, near = pieces(to_group * half + to_local)
            here = (to_group, side * half + to_local)
            across = (to_group, (1 - side) * half + to_local)
            other = (apart > 0) | (step > 0)
            if keys:

                @pl.when(other)
                def _():
                    send(far[0], *here)
                    send(far[1], *here)

                send(far[0], *across)
                send(far[1], *across)
            if queries:

                @pl.when(other)
                def _():
                    send(near[0], *here)
                    send(near[1], *here)

    far, near = pieces(side_slot)
    for source, target, which in far + near[:2]:
        pltpu.make_async_copy(source, target, recv_sem.at[which, group]).start()
    send_group(0, True, True)
    send_group(1, True, False)
    load_grad = pltpu.make_async_copy(grad, grad_own, own_sem.at[0])
    load_out = pltpu.make_async_copy(attn_out, out_own, own_sem.at[1])
    load_grad.start()
    load_out.start()
    load_grad.wait()
    load_out.wait()
    for slot in range(groups * half):
        for part in range(2):
            head = 2 * slot + part
            columns = slice(head * HEAD_SIZE, (head + 1) * HEAD_SIZE)
            both = grad_own[:, columns].astype(jnp.float32) * out_own[:, columns].astype(jnp.float32)
            stat_own[slot, 2 + part : 3 + part] = jnp.sum(both.T, axis=0, keepdims=True)
            stat_own[slot, part : part + 1] = norm[head : head + 1] * math.log2(math.e)
        stat_own[slot, 4:8] = jnp.zeros((4, TOKENS), jnp.float32)

    send_group(groups - 1, True, False)

    @pl.loop(1, groups * half)
    def _(turn):
        to_group = lax.rem(group + turn // half, groups)
        to_local = lax.rem(member + lax.rem(turn, half), half)
        send(pieces(to_group * half + to_local)[1][2], to_group, side * half + to_local)

    keep = pltpu.make_async_copy(stat_own.at[side_slot], stat_all.at[side_slot], recv_sem.at[4, group])
    keep.start()
    send_group(groups - 1, False, True)
    for apart in range(groups - 2, 1, -1):
        send_group(apart, True, True)
    send_group(1, False, True)
    others = (everyone - 1) * TOKENS
    near_others = (groups * half - 1) * TOKENS

    span = members * TOKENS
    per_span = span // 2 // TILE
    parts = TILE // TOKENS
    narrow = pl.ds(pl.multiple_of(side_slot * HEAD_SIZE, HEAD_SIZE), HEAD_SIZE)
    wide = pl.ds(pl.multiple_of(side_slot * 2 * HEAD_SIZE, 2 * HEAD_SIZE), 2 * HEAD_SIZE)

    def compute(at_group, tile):
        first = at_group * span + side * (span // 2) + tile * TILE
        slot = at_group * half + tile * parts
        rows = pl.ds(pl.multiple_of(slot * TOKENS, TOKENS), TILE)
        queries = jnp.concatenate([query_all[rows, :HEAD_SIZE], query_all[rows, HEAD_SIZE:]], 0)
        grads = jnp.concatenate([grad_all[rows, :HEAD_SIZE], grad_all[rows, HEAD_SIZE:]], 0)
        stat = [stat_all[slot + part] for part in range(parts)]
        level = jnp.concatenate([s[h : h + 1] for h in (0, 1) for s in stat], 1)
        delta = jnp.concatenate([s[h : h + 1] for h in (2, 3) for s in stat], 1)
        spot = first + lax.rem(lax.broadcasted_iota(jnp.int32, (1, 2 * TILE), 1), TILE)
        begin = jnp.zeros((1, 2 * TILE), jnp.int32)
        for cut in range(inner):
            bound = offsets[cut + 1]
            begin = jnp.where(spot >= bound, bound, begin)
        sum_q[...] = jnp.zeros_like(sum_q)
        back_blocks = span // TILE

        @pl.loop(0, back_blocks + 1)
        def _(step):
            block = first // TILE + step - back_blocks

            @pl.when(block >= 0)
            def _():
                cols = pl.ds(pl.multiple_of(block * TILE, TILE), TILE)
                score = dot(key_all[cols], queries, ((1,), (1,)))
                where = block * TILE + lax.broadcasted_iota(jnp.int32, (TILE, 2 * TILE), 0)
                allowed = (where >= begin) & (where <= spot)
                power = jnp.exp2(score * (attn_scale * math.log2(math.e)) - level)
                prob = jnp.where(allowed, power, 0.0)
                dprob = dot(value_all[cols], grads, ((1,), (1,)))
                dscore = (prob * (dprob - delta)).astype(jnp.bfloat16)
                sum_v[cols] += dot(prob.astype(jnp.bfloat16), grads, ((1,), (0,)))
                sum_k[cols] += dot(dscore, queries, ((1,), (0,)))
                sum_q[...] += dot(key_turned[block], dscore, ((1,), (0,)))

        for part in (0, 1):
            turned = (sum_q[:, part * TILE : (part + 1) * TILE] * attn_scale).T
            grad_q[rows, part * HEAD_SIZE : (part + 1) * HEAD_SIZE] = turned.astype(jnp.bfloat16)

    def give(piece, to_group, to_member):
        mine = (to_group == group) & (to_member == member)

        @pl.when(mine)
        def _():
            source, target, which = piece
            pltpu.make_async_copy(source, target, recv_sem.at[which, 0]).start()

        @pl.when(jnp.logical_not(mine))
        def _():
            send(piece, to_group, to_member)

    def give_query(at_group, tile):
        for part in range(parts):
            local = tile * parts + part
            row = pl.multiple_of((at_group * half + local) * TOKENS, TOKENS)
            piece = (grad_q.at[pl.ds(row, TOKENS)], query_out.at[:, wide], 5)
            give(piece, at_group, side * half + local)

    def each_owner(chunk, act):
        @pl.loop(0, members)
        def _(step):
            owner = (chunk - 1) * members + side * half + lax.rem(step + member, members)

            @pl.when((owner >= 0) & (owner < everyone))
            def _():
                act(owner, pl.ds(pl.multiple_of(owner * TOKENS, TOKENS), TOKENS))

    def settle(owner, rows):
        grad_k[rows] = (sum_k[rows] * attn_scale).astype(jnp.bfloat16)
        grad_v[rows] = sum_v[rows].astype(jnp.bfloat16)

    def give_key(owner, rows):
        to_group, to_member = owner // members, lax.rem(owner, members)
        give((grad_k.at[rows], key_out.at[side, :, narrow], 6), to_group, to_member)
        give((grad_v.at[rows], value_out.at[side, :, narrow], 7), to_group, to_member)

    def finished(turn, act):
        at_group = lax.rem(group + turn, groups)

        @pl.when((turn > 0) | (at_group == 0))
        def _():
            each_owner(at_group, act)

        @pl.when(at_group == groups - 1)
        def _():
            each_owner(groups, act)

        @pl.when((turn == groups - 1) & (group > 0))
        def _():
            each_owner(group, act)

    def arrive_keys(at_group):
        whole = pl.ds(pl.multiple_of(at_group * span, span), span)
        wait_bytes(key_all.at[whole], recv_sem.at[0, at_group])
        wait_bytes(value_all.at[whole], recv_sem.at[1, at_group])

        @pl.loop(0, span // TILE)
        def _(part):
            block = at_group * (span // TILE) + part
            rows = pl.ds(pl.multiple_of(block * TILE, TILE), TILE)
            key_turned[block] = key_all[rows].T
            sum_k[rows] = jnp.zeros((TILE, HEAD_SIZE), jnp.float32)
            sum_v[rows] = jnp.zeros((TILE, HEAD_SIZE), jnp.float32)

    def arrive_queries(at_group):
        near_span = half * TOKENS
        rows = pl.ds(pl.multiple_of(at_group * near_span, near_span), near_span)
        wait_bytes(query_all.at[rows], recv_sem.at[2, at_group])
        wait_bytes(grad_all.at[rows], recv_sem.at[3, at_group])
        wait_bytes(stat_all.at[pl.ds(at_group * half, half)], recv_sem.at[4, at_group])

    @pl.loop(0, groups)
    def _(turn):
        at_group = lax.rem(group + turn, groups)

        @pl.when((turn < groups - 1) | (group == 0))
        def _():
            arrive_keys(at_group)

        @pl.when((turn == 0) & (group > 0))
        def _():
            arrive_keys(group - 1)

        arrive_queries(at_group)

        @pl.loop(0, per_span)
        def _(part):
            tile = lax.rem(part + lax.rem(member, half) // 2, per_span)
            compute(at_group, tile)

            @pl.when(part > 0)
            def _():
                give_query(at_group, lax.rem(tile + per_span - 1, per_span))

            @pl.when((part == 0) & (turn > 0))
            def _():
                finished(turn - 1, give_key)

        finished(turn, settle)
        last = lax.rem(per_span - 1 + lax.rem(member, half) // 2, per_span)
        give_query(at_group, last)

    finished(groups - 1, give_key)
    wait_bytes(key_all.at[pl.ds(0, others)], send_sem.at[0])
    wait_bytes(value_all.at[pl.ds(0, others)], send_sem.at[1])
    wait_bytes(query_all.at[pl.ds(0, near_others)], send_sem.at[2])
    wait_bytes(grad_all.at[pl.ds(0, near_others)], send_sem.at[3])
    wait_bytes(stat_all.at[pl.ds(0, groups * half - 1)], send_sem.at[4])
    wait_bytes(grad_q.at[pl.ds(0, near_others)], send_sem.at[5])
    wait_bytes(grad_k.at[pl.ds(0, others)], send_sem.at[6])
    wait_bytes(grad_v.at[pl.ds(0, others)], send_sem.at[7])
    wait_bytes(query_out, recv_sem.at[5, 0])
    wait_bytes(key_out, recv_sem.at[6, 0])
    wait_bytes(value_out, recv_sem.at[7, 0])


def dot(left, right, dims):
    return lax.dot_general(left, right, (dims, ((), ())), preferred_element_type=jnp.float32)


def half_shards(
    groups, members, query, key_matrix, value_matrix, output_gradient, attn_out, doc_offsets, stats
):
    slots = groups * (members // 2)
    token_count = groups * members * TOKENS
    near_rows = slots * TOKENS
    low, wide = jnp.bfloat16, jnp.float32
    in_vmem = pl.BlockSpec(memory_space=pltpu.VMEM)
    in_smem = pl.BlockSpec(memory_space=pltpu.SMEM)
    anywhere = pl.BlockSpec(memory_space=pl.ANY)
    grad_query, key_halves, value_halves = pl.pallas_call(
        functools.partial(fused_kernel, groups, members, doc_offsets.shape[0] - 2),
        out_shape=(
            jax.ShapeDtypeStruct((TOKENS, HQ * HEAD_SIZE), low),
            jax.ShapeDtypeStruct((2, TOKENS, slots * HEAD_SIZE), low),
            jax.ShapeDtypeStruct((2, TOKENS, slots * HEAD_SIZE), low),
        ),
        in_specs=[in_smem] + [anywhere] * 5 + [in_vmem],
        out_specs=[anywhere] * 3,
        scratch_shapes=[
            pltpu.VMEM((near_rows, 2 * HEAD_SIZE), low),
            pltpu.VMEM((near_rows, 2 * HEAD_SIZE), low),
            pltpu.VMEM((token_count, HEAD_SIZE), low),
            pltpu.VMEM((token_count, HEAD_SIZE), low),
            pltpu.VMEM((slots, 8, TOKENS), wide),
            pltpu.VMEM((TOKENS, HQ * HEAD_SIZE), low),
            pltpu.VMEM((TOKENS, HQ * HEAD_SIZE), low),
            pltpu.VMEM((slots, 8, TOKENS), wide),
            pltpu.VMEM((near_rows, 2 * HEAD_SIZE), low),
            pltpu.VMEM((token_count, HEAD_SIZE), low),
            pltpu.VMEM((token_count, HEAD_SIZE), low),
            pltpu.VMEM((token_count // TILE, HEAD_SIZE, TILE), low),
            pltpu.VMEM((HEAD_SIZE, 2 * TILE), wide),
            pltpu.VMEM((token_count, HEAD_SIZE), wide),
            pltpu.VMEM((token_count, HEAD_SIZE), wide),
            pltpu.SemaphoreType.DMA((8,)),
            pltpu.SemaphoreType.DMA((8, groups)),
            pltpu.SemaphoreType.DMA((2,)),
        ],
        compiler_params=pltpu.CompilerParams(
            collective_id=0, has_side_effects=True
        ),
        name="fused",
    )(doc_offsets, query, output_gradient, key_matrix, value_matrix, attn_out, stats.T)
    key_gradient = (key_halves[0].astype(wide) + key_halves[1].astype(wide)).astype(low)
    value_gradient = (value_halves[0].astype(wide) + value_halves[1].astype(wide)).astype(low)
    return (grad_query, key_gradient, value_gradient)


def solution(mesh):
    placed = (
        P(("seq", "head"), None),
        P(("seq", "head"), None),
        P(("seq", "head"), None),
        P(("seq", "head"), None),
        P(("seq", "head"), None),
        P(),
        P(("seq", "head"), None),
    )
    groups, members = mesh.shape["seq"], mesh.shape["head"]
    halves_fit = groups > 2 and members % 2 == 0 and groups * (members // 2) * 2 == HQ

    def whole(*arrays):
        tokens = arrays[0].shape[0] // (groups * members)
        fits = halves_fit and tokens == TOKENS and tokens * members == 2 * DOCHALF
        body = functools.partial(half_shards, groups, members) if fits else shards
        return mapped(body)(*arrays)

    def mapped(body):
        return jax.shard_map(
            body,
            mesh=mesh,
            in_specs=placed,
            out_specs=(P(("seq", "head"), None), P(("seq", "head"), None), P(("seq", "head"), None)),
            check_vma=False,
        )

    return whole
```

```python
import functools
import math

import jax
import jax.numpy as jnp
from jax import lax
from jax.experimental import pallas as pl
from jax.experimental.pallas import tpu as pltpu
from jax.sharding import PartitionSpec as P

HQ = 32
HEAD_SIZE = 128
DOCHALF = 512
QBLK = 512


attn_scale = 144.0 ** (-0.5)


def partner(value, axis, apart):
    mask = 2**apart
    pairs = [(source, source ^ mask) for source in range(lax.axis_size(axis))]
    return lax.ppermute(value, axis, pairs)


def from_behind(value, axis, steps):
    count = lax.axis_size(axis)
    leading, last = (max(0, -steps), min(count, count - steps))
    return lax.ppermute(value, axis, [(source, source + steps) for source in range(leading, last)])


def tile_grads(query_rows, grad_rows, lse_rows, delta_rows, key_window, value_window, allowed):
    score = (
        jnp.einsum("qgrd,kgd->grqk", query_rows, key_window, preferred_element_type=jnp.float32)
        * attn_scale
    )
    norm_stat = jnp.transpose(lse_rows, (1, 2, 0))[..., None]
    prob = jnp.where(allowed[None, None], jnp.exp(score - norm_stat), 0.0)
    dprob = jnp.einsum(
        "qgrd,kgd->grqk", grad_rows, value_window, preferred_element_type=jnp.float32
    )
    dscore = prob * (dprob - jnp.transpose(delta_rows, (1, 2, 0))[..., None])
    prob_low = prob.astype(jnp.bfloat16)
    dscore_low = dscore.astype(jnp.bfloat16)
    value_gradient = jnp.einsum(
        "grqk,qgrd->kgd", prob_low, grad_rows, preferred_element_type=jnp.float32
    )
    key_gradient = (
        jnp.einsum("grqk,qgrd->kgd", dscore_low, query_rows, preferred_element_type=jnp.float32)
        * attn_scale
    )
    grad_query = (
        jnp.einsum("grqk,kgd->qgrd", dscore_low, key_window, preferred_element_type=jnp.float32)
        * attn_scale
    )
    return (grad_query, key_gradient, value_gradient)


def doc_numbers(positions, inner):
    return jnp.sum((inner[None, :] <= positions[:, None]).astype(jnp.int32), axis=1)


def shards(query, key_matrix, value_matrix, output_gradient, attn_out, doc_offsets, stats):
    token_count_local = query.shape[0]
    members = lax.axis_size("head")
    group_span = token_count_local * members
    per_device = HQ // members
    lookback = 2 * DOCHALF
    width = lookback + QBLK
    group = lax.axis_index("seq")
    member = lax.axis_index("head")
    parity = member % 2
    half_width = HEAD_SIZE // 2
    delta_correction = jnp.sum(
        (output_gradient.astype(jnp.float32) * attn_out.astype(jnp.float32)).reshape(
            token_count_local, HQ, HEAD_SIZE
        ),
        axis=2,
    )
    query_heads, grad_heads = (
        lax.all_to_all(query, "head", split_axis=1, concat_axis=0, tiled=True),
        lax.all_to_all(output_gradient, "head", split_axis=1, concat_axis=0, tiled=True),
    )
    lse_heads, delta_heads = (
        lax.all_to_all(stats, "head", split_axis=1, concat_axis=0, tiled=True),
        lax.all_to_all(delta_correction, "head", split_axis=1, concat_axis=0, tiled=True),
    )
    key_cols, value_cols = (
        lax.all_to_all(key_matrix, "head", split_axis=1, concat_axis=0, tiled=True),
        lax.all_to_all(value_matrix, "head", split_axis=1, concat_axis=0, tiled=True),
    )
    if per_device >= 2:
        groups = per_device // 2
        key_heads = key_cols.reshape(group_span, groups, HEAD_SIZE)
        value_heads = value_cols.reshape(group_span, groups, HEAD_SIZE)
    else:
        groups = 1
        other_key, other_value = partner((key_cols, value_cols), "head", 0)
        key_heads = jnp.where(
            parity == 0,
            jnp.concatenate([key_cols, other_key], 1),
            jnp.concatenate([other_key, key_cols], 1),
        ).reshape(group_span, 1, HEAD_SIZE)
        value_heads = jnp.where(
            parity == 0,
            jnp.concatenate([value_cols, other_value], 1),
            jnp.concatenate([other_value, value_cols], 1),
        ).reshape(group_span, 1, HEAD_SIZE)
    repeats = per_device // groups
    query_heads = query_heads.reshape(group_span, groups, repeats, HEAD_SIZE)
    grad_heads = grad_heads.reshape(group_span, groups, repeats, HEAD_SIZE)
    lse_heads = lse_heads.reshape(group_span, groups, repeats)
    delta_heads = delta_heads.reshape(group_span, groups, repeats)
    prior_key, prior_value = from_behind(
        (key_heads[group_span - lookback :], value_heads[group_span - lookback :]), "seq", 1
    )
    key_ext = jnp.concatenate([prior_key, key_heads], 0)
    value_ext = jnp.concatenate([prior_value, value_heads], 0)
    inner = doc_offsets[1:-1]
    query_pos = group * group_span + jnp.arange(group_span, dtype=jnp.int32)
    key_pos = group * group_span - lookback + jnp.arange(lookback + group_span, dtype=jnp.int32)
    query_doc = doc_numbers(query_pos, inner)
    key_doc = doc_numbers(key_pos, inner)

    def block_step(block, carry):
        grad_q, grad_k, grad_v = carry
        start = (block * QBLK).astype(jnp.int32)
        query_rows = lax.dynamic_slice_in_dim(query_heads, start, QBLK, 0)
        grad_rows = lax.dynamic_slice_in_dim(grad_heads, start, QBLK, 0)
        lse_rows = lax.dynamic_slice_in_dim(lse_heads, start, QBLK, 0)
        delta_rows = lax.dynamic_slice_in_dim(delta_heads, start, QBLK, 0)
        key_window = lax.dynamic_slice_in_dim(key_ext, start, width, 0)
        value_window = lax.dynamic_slice_in_dim(value_ext, start, width, 0)
        rows_pos = lax.dynamic_slice_in_dim(query_pos, start, QBLK, 0)
        rows_doc = lax.dynamic_slice_in_dim(query_doc, start, QBLK, 0)
        cols_pos = lax.dynamic_slice_in_dim(key_pos, start, width, 0)
        cols_doc = lax.dynamic_slice_in_dim(key_doc, start, width, 0)
        allowed = (
            (cols_doc[None, :] == rows_doc[:, None])
            & (cols_pos[None, :] <= rows_pos[:, None])
            & (cols_pos[None, :] >= 0)
        )
        block_q, block_k, block_v = tile_grads(
            query_rows, grad_rows, lse_rows, delta_rows, key_window, value_window, allowed
        )
        grad_q = lax.dynamic_update_slice_in_dim(grad_q, block_q, start, 0)
        grad_k = lax.dynamic_update_slice_in_dim(
            grad_k, lax.dynamic_slice_in_dim(grad_k, start, width, 0) + block_k, start, 0
        )
        grad_v = lax.dynamic_update_slice_in_dim(
            grad_v, lax.dynamic_slice_in_dim(grad_v, start, width, 0) + block_v, start, 0
        )
        return (grad_q, grad_k, grad_v)

    init = (
        jnp.zeros((group_span, groups, repeats, HEAD_SIZE), jnp.float32),
        jnp.zeros((lookback + group_span, groups, HEAD_SIZE), jnp.float32),
        jnp.zeros((lookback + group_span, groups, HEAD_SIZE), jnp.float32),
    )
    grad_q, grad_k, grad_v = lax.fori_loop(0, group_span // QBLK, block_step, init)
    back_key, back_value = (
        from_behind(grad_k[:lookback].astype(jnp.bfloat16), "seq", -1).astype(jnp.float32),
        from_behind(grad_v[:lookback].astype(jnp.bfloat16), "seq", -1).astype(jnp.float32),
    )
    own_key = grad_k[lookback:].at[group_span - lookback :].add(back_key)
    own_value = grad_v[lookback:].at[group_span - lookback :].add(back_value)
    query_low = grad_q.astype(jnp.bfloat16).reshape(group_span, per_device * HEAD_SIZE)
    grad_query = lax.all_to_all(query_low, "head", split_axis=0, concat_axis=1, tiled=True)
    if per_device >= 2:
        send_key = own_key.reshape(group_span, groups * HEAD_SIZE)
        send_value = own_value.reshape(group_span, groups * HEAD_SIZE)
    else:
        flat_key = own_key.reshape(group_span, HEAD_SIZE)
        flat_value = own_value.reshape(group_span, HEAD_SIZE)
        keep_key = lax.dynamic_slice_in_dim(flat_key, parity * half_width, half_width, 1)
        keep_value = lax.dynamic_slice_in_dim(flat_value, parity * half_width, half_width, 1)
        give_key = lax.dynamic_slice_in_dim(flat_key, (1 - parity) * half_width, half_width, 1)
        give_value = lax.dynamic_slice_in_dim(flat_value, (1 - parity) * half_width, half_width, 1)
        from_key, from_value = partner((give_key, give_value), "head", 0)
        send_key = keep_key + from_key
        send_value = keep_value + from_value
    key_gradient_summed, value_gradient_summed = (
        lax.all_to_all(
            send_key.astype(jnp.bfloat16), "head", split_axis=0, concat_axis=1, tiled=True
        ).astype(send_key.dtype),
        lax.all_to_all(
            send_value.astype(jnp.bfloat16), "head", split_axis=0, concat_axis=1, tiled=True
        ).astype(send_value.dtype),
    )
    key_gradient = key_gradient_summed.astype(jnp.bfloat16)
    value_gradient = value_gradient_summed.astype(jnp.bfloat16)
    return (grad_query, key_gradient, value_gradient)


TOKENS = 128
TILE = 256
MESH = pl.DeviceIdType.MESH


def wait_bytes(ref, sem):
    pltpu.make_async_copy(ref, ref, sem).wait()


def greet_all(groups, members, group, member):
    barrier = pltpu.get_barrier_semaphore()
    everyone = groups * members

    @pl.loop(1, everyone)
    def _(apart):
        to_group = lax.rem(group + apart // members, groups)
        to_member = lax.rem(member + lax.rem(apart, members), members)
        pl.semaphore_signal(barrier, inc=1, device_id=(to_group, to_member), device_id_type=MESH)

    pl.semaphore_wait(barrier, everyone - 1)


def fused_kernel(
    groups,
    members,
    inner,
    offsets,
    query,
    grad,
    key,
    value,
    attn_out,
    norm,
    query_out,
    key_out,
    value_out,
    query_all,
    grad_all,
    key_all,
    value_all,
    stat_all,
    grad_own,
    out_own,
    stat_own,
    grad_q,
    grad_k,
    grad_v,
    key_turned,
    sum_q,
    sum_k,
    sum_v,
    send_sem,
    recv_sem,
    own_sem,
):
    half = members // 2
    everyone = groups * members
    group = lax.axis_index("seq")
    member = lax.axis_index("head")
    side = member // half
    greet_all(groups, members, group, member)
    tail_rows = (group == groups - 1) & (side == 1)
    token_row = pl.multiple_of((group * members + member) * TOKENS, TOKENS)
    side_slot = group * half + lax.rem(member, half)
    side_row = pl.multiple_of(side_slot * TOKENS, TOKENS)

    def pieces(slot):
        narrow = pl.ds(pl.multiple_of(slot * HEAD_SIZE, HEAD_SIZE), HEAD_SIZE)
        wide = pl.ds(pl.multiple_of(slot * 2 * HEAD_SIZE, 2 * HEAD_SIZE), 2 * HEAD_SIZE)
        far = (
            (key.at[:, narrow], key_all.at[pl.ds(token_row, TOKENS)], 0),
            (value.at[:, narrow], value_all.at[pl.ds(token_row, TOKENS)], 1),
        )
        near = (
            (query.at[:, wide], query_all.at[pl.ds(side_row, TOKENS)], 2),
            (grad.at[:, wide], grad_all.at[pl.ds(side_row, TOKENS)], 3),
            (stat_own.at[slot], stat_all.at[side_slot], 4),
        )
        return far, near

    def slot_of(which):
        return group if which < 5 else 0

    def send(piece, to_group, to_member):
        source, target, which = piece
        pltpu.make_async_remote_copy(
            src_ref=source,
            dst_ref=target,
            send_sem=send_sem.at[which],
            recv_sem=recv_sem.at[which, slot_of(which)],
            device_id=(to_group, to_member),
            device_id_type=MESH,
        ).start()

    def send_group(apart, keys, queries):
        to_group = lax.rem(group + apart, groups)

        @pl.loop(0, half)
        def _(step):
            to_local = lax.rem(member + step, half)
            far, near = pieces(to_group * half + to_local)
            here = (to_group, side * half + to_local)
            across = (to_group, (1 - side) * half + to_local)
            other = (apart > 0) | (step > 0)
            if keys:

                @pl.when(other)
                def _():
                    send(far[0], *here)
                    send(far[1], *here)

                @pl.when(jnp.logical_not(tail_rows))
                def _():
                    send(far[0], *across)
                    send(far[1], *across)

            if queries:

                @pl.when(other)
                def _():
                    send(near[0], *here)
                    send(near[1], *here)

    far, near = pieces(side_slot)
    for source, target, which in far + near[:2]:
        pltpu.make_async_copy(source, target, recv_sem.at[which, group]).start()
    send_group(0, True, True)
    send_group(1, True, False)
    load_grad = pltpu.make_async_copy(grad, grad_own, own_sem.at[0])
    load_out = pltpu.make_async_copy(attn_out, out_own, own_sem.at[1])
    load_grad.start()
    load_out.start()
    load_grad.wait()
    load_out.wait()
    for slot in range(groups * half):
        for part in range(2):
            head = 2 * slot + part
            columns = slice(head * HEAD_SIZE, (head + 1) * HEAD_SIZE)
            both = grad_own[:, columns].astype(jnp.float32) * out_own[:, columns].astype(jnp.float32)
            stat_own[slot, 2 + part : 3 + part] = jnp.sum(both.T, axis=0, keepdims=True)
            stat_own[slot, part : part + 1] = norm[head : head + 1] * math.log2(math.e)
        stat_own[slot, 4:8] = jnp.zeros((4, TOKENS), jnp.float32)

    send_group(groups - 1, True, False)

    @pl.loop(1, groups * half)
    def _(turn):
        to_group = lax.rem(group + turn // half, groups)
        to_local = lax.rem(member + lax.rem(turn, half), half)
        send(pieces(to_group * half + to_local)[1][2], to_group, side * half + to_local)

    keep = pltpu.make_async_copy(stat_own.at[side_slot], stat_all.at[side_slot], recv_sem.at[4, group])
    keep.start()
    send_group(groups - 1, False, True)
    for apart in range(groups - 2, 1, -1):
        send_group(apart, True, True)
    send_group(1, False, True)
    others = (everyone - 1) * TOKENS
    near_others = (groups * half - 1) * TOKENS

    span = members * TOKENS
    per_span = span // 2 // TILE
    parts = TILE // TOKENS
    narrow = pl.ds(pl.multiple_of(side_slot * HEAD_SIZE, HEAD_SIZE), HEAD_SIZE)
    wide = pl.ds(pl.multiple_of(side_slot * 2 * HEAD_SIZE, 2 * HEAD_SIZE), 2 * HEAD_SIZE)

    def compute(at_group, tile):
        first = at_group * span + side * (span // 2) + tile * TILE
        slot = at_group * half + tile * parts
        rows = pl.ds(pl.multiple_of(slot * TOKENS, TOKENS), TILE)
        queries = jnp.concatenate([query_all[rows, :HEAD_SIZE], query_all[rows, HEAD_SIZE:]], 0)
        grads = jnp.concatenate([grad_all[rows, :HEAD_SIZE], grad_all[rows, HEAD_SIZE:]], 0)
        stat = [stat_all[slot + part] for part in range(parts)]
        level = jnp.concatenate([s[h : h + 1] for h in (0, 1) for s in stat], 1)
        delta = jnp.concatenate([s[h : h + 1] for h in (2, 3) for s in stat], 1)
        spot = first + lax.rem(lax.broadcasted_iota(jnp.int32, (1, 2 * TILE), 1), TILE)
        begin = jnp.zeros((1, 2 * TILE), jnp.int32)
        for cut in range(inner):
            bound = offsets[cut + 1]
            begin = jnp.where(spot >= bound, bound, begin)
        sum_q[...] = jnp.zeros_like(sum_q)
        back_blocks = span // TILE

        @pl.loop(0, back_blocks + 1)
        def _(step):
            block = first // TILE + step - back_blocks

            @pl.when(block >= 0)
            def _():
                cols = pl.ds(pl.multiple_of(block * TILE, TILE), TILE)
                score = dot(key_all[cols], queries, ((1,), (1,)))
                where = block * TILE + lax.broadcasted_iota(jnp.int32, (TILE, 2 * TILE), 0)
                allowed = (where >= begin) & (where <= spot)
                power = jnp.exp2(score * (attn_scale * math.log2(math.e)) - level)
                prob = jnp.where(allowed, power, 0.0)
                dprob = dot(value_all[cols], grads, ((1,), (1,)))
                dscore = (prob * (dprob - delta)).astype(jnp.bfloat16)
                sum_v[cols] += dot(prob.astype(jnp.bfloat16), grads, ((1,), (0,)))
                sum_k[cols] += dot(dscore, queries, ((1,), (0,)))
                sum_q[...] += dot(key_turned[block], dscore, ((1,), (0,)))

        for part in (0, 1):
            turned = (sum_q[:, part * TILE : (part + 1) * TILE] * attn_scale).T
            grad_q[rows, part * HEAD_SIZE : (part + 1) * HEAD_SIZE] = turned.astype(jnp.bfloat16)

    def give(piece, to_group, to_member):
        mine = (to_group == group) & (to_member == member)

        @pl.when(mine)
        def _():
            source, target, which = piece
            pltpu.make_async_copy(source, target, recv_sem.at[which, 0]).start()

        @pl.when(jnp.logical_not(mine))
        def _():
            send(piece, to_group, to_member)

    def give_query(at_group, tile):
        for part in range(parts):
            local = tile * parts + part
            row = pl.multiple_of((at_group * half + local) * TOKENS, TOKENS)
            piece = (grad_q.at[pl.ds(row, TOKENS)], query_out.at[:, wide], 5)
            give(piece, at_group, side * half + local)

    def each_owner(chunk, act):
        @pl.loop(0, members)
        def _(step):
            owner = (chunk - 1) * members + side * half + lax.rem(step + member, members)

            @pl.when((owner >= 0) & (owner < everyone - (1 - side) * half))
            def _():
                act(owner, pl.ds(pl.multiple_of(owner * TOKENS, TOKENS), TOKENS))

    def settle(owner, rows):
        grad_k[rows] = (sum_k[rows] * attn_scale).astype(jnp.bfloat16)
        grad_v[rows] = sum_v[rows].astype(jnp.bfloat16)

    def give_key(owner, rows):
        to_group, to_member = owner // members, lax.rem(owner, members)
        give((grad_k.at[rows], key_out.at[side, :, narrow], 6), to_group, to_member)
        give((grad_v.at[rows], value_out.at[side, :, narrow], 7), to_group, to_member)

    def finished(turn, act):
        at_group = lax.rem(group + turn, groups)

        @pl.when((turn > 0) | (at_group == 0))
        def _():
            each_owner(at_group, act)

        @pl.when(at_group == groups - 1)
        def _():
            each_owner(groups, act)

        @pl.when((turn == groups - 1) & (group > 0))
        def _():
            each_owner(group, act)

    def arrive_keys(at_group):
        whole = pl.ds(pl.multiple_of(at_group * span, span), span)
        first_half = pl.ds(pl.multiple_of(at_group * span, span), span // 2)
        part_only = (at_group == groups - 1) & (side == 0)

        @pl.when(part_only)
        def _():
            wait_bytes(key_all.at[first_half], recv_sem.at[0, at_group])
            wait_bytes(value_all.at[first_half], recv_sem.at[1, at_group])

        @pl.when(jnp.logical_not(part_only))
        def _():
            wait_bytes(key_all.at[whole], recv_sem.at[0, at_group])
            wait_bytes(value_all.at[whole], recv_sem.at[1, at_group])

        @pl.loop(0, span // TILE)
        def _(part):
            block = at_group * (span // TILE) + part
            rows = pl.ds(pl.multiple_of(block * TILE, TILE), TILE)

            @pl.when(jnp.logical_not(part_only) | (part < span // TILE // 2))
            def _():
                key_turned[block] = key_all[rows].T

            sum_k[rows] = jnp.zeros((TILE, HEAD_SIZE), jnp.float32)
            sum_v[rows] = jnp.zeros((TILE, HEAD_SIZE), jnp.float32)

    def arrive_queries(at_group):
        near_span = half * TOKENS
        rows = pl.ds(pl.multiple_of(at_group * near_span, near_span), near_span)
        wait_bytes(query_all.at[rows], recv_sem.at[2, at_group])
        wait_bytes(grad_all.at[rows], recv_sem.at[3, at_group])
        wait_bytes(stat_all.at[pl.ds(at_group * half, half)], recv_sem.at[4, at_group])

    @pl.loop(0, groups)
    def _(turn):
        at_group = lax.rem(group + turn, groups)

        @pl.when((turn < groups - 1) | (group == 0))
        def _():
            arrive_keys(at_group)

        @pl.when((turn == 0) & (group > 0))
        def _():
            arrive_keys(group - 1)

        arrive_queries(at_group)

        @pl.loop(0, per_span)
        def _(part):
            tile = lax.rem(part + lax.rem(member, half) // 2, per_span)
            compute(at_group, tile)

            @pl.when(part > 0)
            def _():
                give_query(at_group, lax.rem(tile + per_span - 1, per_span))

            @pl.when((part == 0) & (turn > 0))
            def _():
                finished(turn - 1, give_key)

        finished(turn, settle)
        last = lax.rem(per_span - 1 + lax.rem(member, half) // 2, per_span)
        give_query(at_group, last)

    finished(groups - 1, give_key)
    for which, ref in enumerate((key_all, value_all)):

        @pl.when(tail_rows)
        def _():
            wait_bytes(ref.at[pl.ds(0, near_others)], send_sem.at[which])

        @pl.when(jnp.logical_not(tail_rows))
        def _():
            wait_bytes(ref.at[pl.ds(0, others)], send_sem.at[which])

    wait_bytes(query_all.at[pl.ds(0, near_others)], send_sem.at[2])
    wait_bytes(grad_all.at[pl.ds(0, near_others)], send_sem.at[3])
    wait_bytes(stat_all.at[pl.ds(0, groups * half - 1)], send_sem.at[4])
    wait_bytes(grad_q.at[pl.ds(0, near_others)], send_sem.at[5])
    for which, ref in ((6, grad_k), (7, grad_v)):

        @pl.when(side == 0)
        def _():
            wait_bytes(ref.at[pl.ds(0, others - half * TOKENS)], send_sem.at[which])

        @pl.when(side == 1)
        def _():
            wait_bytes(ref.at[pl.ds(0, others)], send_sem.at[which])

    wait_bytes(query_out, recv_sem.at[5, 0])
    for which, ref in ((6, key_out), (7, value_out)):

        @pl.when(tail_rows)
        def _():
            wait_bytes(ref.at[1], recv_sem.at[which, 0])

        @pl.when(jnp.logical_not(tail_rows))
        def _():
            wait_bytes(ref, recv_sem.at[which, 0])


def dot(left, right, dims):
    return lax.dot_general(left, right, (dims, ((), ())), preferred_element_type=jnp.float32)


def half_shards(
    groups, members, query, key_matrix, value_matrix, output_gradient, attn_out, doc_offsets, stats
):
    slots = groups * (members // 2)
    token_count = groups * members * TOKENS
    near_rows = slots * TOKENS
    low, wide = jnp.bfloat16, jnp.float32
    in_vmem = pl.BlockSpec(memory_space=pltpu.VMEM)
    in_smem = pl.BlockSpec(memory_space=pltpu.SMEM)
    anywhere = pl.BlockSpec(memory_space=pl.ANY)
    grad_query, key_halves, value_halves = pl.pallas_call(
        functools.partial(fused_kernel, groups, members, doc_offsets.shape[0] - 2),
        out_shape=(
            jax.ShapeDtypeStruct((TOKENS, HQ * HEAD_SIZE), low),
            jax.ShapeDtypeStruct((2, TOKENS, slots * HEAD_SIZE), low),
            jax.ShapeDtypeStruct((2, TOKENS, slots * HEAD_SIZE), low),
        ),
        in_specs=[in_smem] + [anywhere] * 5 + [in_vmem],
        out_specs=[anywhere] * 3,
        scratch_shapes=[
            pltpu.VMEM((near_rows, 2 * HEAD_SIZE), low),
            pltpu.VMEM((near_rows, 2 * HEAD_SIZE), low),
            pltpu.VMEM((token_count, HEAD_SIZE), low),
            pltpu.VMEM((token_count, HEAD_SIZE), low),
            pltpu.VMEM((slots, 8, TOKENS), wide),
            pltpu.VMEM((TOKENS, HQ * HEAD_SIZE), low),
            pltpu.VMEM((TOKENS, HQ * HEAD_SIZE), low),
            pltpu.VMEM((slots, 8, TOKENS), wide),
            pltpu.VMEM((near_rows, 2 * HEAD_SIZE), low),
            pltpu.VMEM((token_count, HEAD_SIZE), low),
            pltpu.VMEM((token_count, HEAD_SIZE), low),
            pltpu.VMEM((token_count // TILE, HEAD_SIZE, TILE), low),
            pltpu.VMEM((HEAD_SIZE, 2 * TILE), wide),
            pltpu.VMEM((token_count, HEAD_SIZE), wide),
            pltpu.VMEM((token_count, HEAD_SIZE), wide),
            pltpu.SemaphoreType.DMA((8,)),
            pltpu.SemaphoreType.DMA((8, groups)),
            pltpu.SemaphoreType.DMA((2,)),
        ],
        compiler_params=pltpu.CompilerParams(
            collective_id=0, has_side_effects=True
        ),
        name="fused",
    )(doc_offsets, query, output_gradient, key_matrix, value_matrix, attn_out, stats.T)
    lone = (lax.axis_index("seq") == groups - 1) & (lax.axis_index("head") >= members // 2)

    def total(halves):
        return (jnp.where(lone, 0.0, halves[0].astype(wide)) + halves[1].astype(wide)).astype(low)

    key_gradient, value_gradient = total(key_halves), total(value_halves)
    return (grad_query, key_gradient, value_gradient)


def solution(mesh):
    placed = (
        P(("seq", "head"), None),
        P(("seq", "head"), None),
        P(("seq", "head"), None),
        P(("seq", "head"), None),
        P(("seq", "head"), None),
        P(),
        P(("seq", "head"), None),
    )
    groups, members = mesh.shape["seq"], mesh.shape["head"]
    halves_fit = groups > 2 and members % 2 == 0 and groups * (members // 2) * 2 == HQ

    def whole(*arrays):
        tokens = arrays[0].shape[0] // (groups * members)
        fits = halves_fit and tokens == TOKENS and tokens * members == 2 * DOCHALF
        body = functools.partial(half_shards, groups, members) if fits else shards
        return mapped(body)(*arrays)

    def mapped(body):
        return jax.shard_map(
            body,
            mesh=mesh,
            in_specs=placed,
            out_specs=(P(("seq", "head"), None), P(("seq", "head"), None), P(("seq", "head"), None)),
            check_vma=False,
        )

    return whole
```
